32 devices in a mesh: dp: 4 (over y, z), tp: 8 (over x, core).
Axes of the slice: x: 4, y: 2, z: 2, core: 2. Of those that a mesh axis runs over, the one named last changes fastest.
The devices are a block of a 4x4x8 slice.
Arguments:
- token_ids: int32 [4, 8192], P('dp'), parts along dimension 0
- emb_table: bfloat16 [32000, 2048], P('tp')
- norm_gain: bfloat16 [2048], replicated
- grad_out: bfloat16 [4, 8192, 2048], P('dp', 'tp'), parts along dimension 0
Outputs:
- output 1: bfloat16 [4, 8192, 2048], P('dp', 'tp'), parts along dimension 0
- output 2: float32 [128000, 2048], P(('dp', 'tp')), parts along dimension 0
- output 3: float32 [8192], P('dp'), parts along dimension 0
There are 4 independent parts. The reference program is written for one: setup_inputs(seed, part) draws one part's arguments, and reference() takes and returns one part's arrays. A program takes and returns all parts, laid end to end along the dimension named above; an argument that names none is the same for every part.
All inputs are finite; a program needn't handle non-finite values.
Results may differ from the reference program's by a relative error of at most 0.00852753.
Values are sent between devices in bfloat16 or wider.
A program may use at most 768 MiB of HBM per device.

```python
import jax
import jax.numpy as jnp
from jax import lax

VOCAB_SIZE = 32000
HIDDEN = 2048
BATCH_ROWS = 1
SEQ_LEN = 8192
RMS_EPS = 1e-5


def setup_inputs(seed: int = 0, part: int = 0) -> dict:
    base_key = jax.random.key(seed)
    key_table, key_gain, key_perm, key_ids, key_grad = jax.random.split(base_key, 5)
    popularity = jax.random.permutation(key_perm, VOCAB_SIZE)
    uniform_draws = jax.random.randint(jax.random.fold_in(key_ids, part), (BATCH_ROWS, SEQ_LEN), 1, 1048577)
    ranks = (67108864 // uniform_draws - 64) % VOCAB_SIZE
    token_ids = jnp.take(popularity, ranks).astype(jnp.int32)
    token_ids = token_ids.at[0, 0].set(0).at[BATCH_ROWS - 1, SEQ_LEN - 1].set(VOCAB_SIZE - 1)
    emb_table = jax.random.normal(key_table, (VOCAB_SIZE, HIDDEN), jnp.float32).astype(jnp.bfloat16)
    norm_gain = (1.0 + 0.5 * jax.random.normal(key_gain, (HIDDEN,), jnp.float32)).astype(jnp.bfloat16)
    grad_out = jax.random.normal(jax.random.fold_in(key_grad, part), (BATCH_ROWS, SEQ_LEN, HIDDEN), jnp.float32).astype(jnp.bfloat16)
    return {'token_ids': token_ids, 'emb_table': emb_table, 'norm_gain': norm_gain, 'grad_out': grad_out}


def reference(token_ids, emb_table, norm_gain, grad_out):
    embedded = jnp.take(emb_table, token_ids, axis=0)
    hidden_f32 = embedded.astype(jnp.float32)
    inv_rms = lax.rsqrt(jnp.mean(hidden_f32 * hidden_f32, axis=-1, keepdims=True) + RMS_EPS)
    x_hat = hidden_f32 * inv_rms
    normed = x_hat.astype(jnp.bfloat16) * norm_gain
    grad_f32 = grad_out.astype(jnp.float32)
    grad_gain = jnp.sum(grad_f32 * x_hat, axis=(0, 1))
    grad_hat = grad_f32 * norm_gain.astype(jnp.float32)
    grad_in = inv_rms * (grad_hat - x_hat * jnp.mean(grad_hat * x_hat, axis=-1, keepdims=True))
    grad_rows = grad_in.astype(jnp.bfloat16).astype(jnp.float32).reshape(-1, HIDDEN)
    grad_table = jax.ops.segment_sum(grad_rows, token_ids.reshape(-1), num_segments=VOCAB_SIZE)
    return normed, grad_table, grad_gain
```

```python
import functools

import jax
import jax.numpy as jnp
from jax import lax
from jax.experimental import pallas as pl
from jax.experimental.pallas import tpu as pltpu
from jax.sharding import PartitionSpec as P

RMS_EPS = 1e-5
MESH = pl.DeviceIdType.MESH
LANES = 128
CORES = 2
CAP = 112
CODE = 256
NT = (((1,), (1,)), ((), ()))
TN = (((0,), (0,)), ((), ()))
F32, BF16 = jnp.float32, jnp.bfloat16


def onehot(mask):
    return jnp.where(mask, 1.0, 0.0).astype(BF16)


def lists_kernel(n, rows, ids_ref, uid_ref, code_ref, top_ref, rank_ref):
    m, width = ids_ref.shape
    hb = -(-rows // LANES)
    high = n * hb
    me = lax.axis_index('tp')
    chip = me // CORES

    def split(ids):
        owner = jnp.zeros_like(ids)
        for k in range(1, n):
            owner += (ids >= k * rows).astype(jnp.int32)
        local = ids - owner * rows
        return owner, owner * hb + (local >> 7), local & (LANES - 1)

    def hots(hi, lo):
        h = onehot(lax.broadcasted_iota(jnp.int32, (high, width), 0) == hi)
        l = onehot(lax.broadcasted_iota(jnp.int32, (LANES, width), 0) == lo)
        return h, l

    a = lax.broadcasted_iota(jnp.int32, (LANES, LANES), 0)
    b = lax.broadcasted_iota(jnp.int32, (LANES, LANES), 1)
    upper, ones = onehot(a <= b), jnp.ones((LANES, LANES), BF16)
    ra = lax.broadcasted_iota(jnp.int32, (high, high), 0)
    rb = lax.broadcasted_iota(jnp.int32, (high, high), 1)
    first = jnp.zeros_like(ra)
    for k in range(1, n):
        first += jnp.where(ra >= k * hb, hb, 0)
    before = onehot((rb < ra) & (rb >= first))

    top = jnp.full((high, LANES), -1.0, F32)
    for j in range(m):
        _, hi, lo = split(ids_ref[j:j + 1, :])
        h, l = hots(hi, lo)
        count = lax.dot_general(h, l, NT, preferred_element_type=F32)
        here = count > 0.5
        present = onehot(here)
        upto = jnp.dot(present, upper, preferred_element_type=F32)
        total = jnp.dot(present, ones, preferred_element_type=F32).astype(BF16)
        base = jnp.dot(before, total, preferred_element_type=F32)
        rank = jnp.where(here, base + upto - 1.0, -1.0)
        top = jnp.maximum(top, rank)
        rank_ref[j] = jnp.minimum(rank, CODE - 1.0)
    top_ref[...] = jnp.broadcast_to(jnp.max(top, axis=(0, 1), keepdims=True), top_ref.shape)

    owner, hi, lo = split(ids_ref[pl.ds(chip, 1), :])
    h, l = hots(hi, lo)
    picked = lax.dot_general(rank_ref[chip].astype(BF16), h, TN, preferred_element_type=F32)
    place = jnp.sum(picked * l.astype(F32), axis=0, keepdims=True)
    code_ref[...] = owner.astype(F32) * CODE + place

    want = lax.broadcasted_iota(jnp.int32, (CAP, LANES), 0).astype(F32)
    lane = lax.broadcasted_iota(jnp.int32, (1, LANES), 1)
    for j in range(m):
        mine = rank_ref[j, pl.ds(pl.multiple_of(me * hb, hb), hb), :]
        found = jnp.zeros((CAP, LANES), jnp.int32)
        for k in range(hb):
            found += jnp.where(mine[k:k + 1, :] == want, k * LANES + lane, 0)
        ids = jnp.sum(found.astype(F32), axis=1, keepdims=True).astype(jnp.int32)
        uid_ref[j * CAP:(j + 1) * CAP, :] = jnp.broadcast_to(ids, (CAP, LANES))


def make_lists(token_ids, n, rows):
    m = n // CORES
    ids = token_ids.reshape(m, -1)
    hb = -(-rows // LANES)
    vm = pl.BlockSpec(memory_space=pltpu.VMEM)
    return pl.pallas_call(
        functools.partial(lists_kernel, n, rows),
        out_shape=(
            jax.ShapeDtypeStruct((m * CAP, LANES), jnp.int32),
            jax.ShapeDtypeStruct((1, ids.shape[1]), F32),
            jax.ShapeDtypeStruct((8, LANES), F32),
        ),
        in_specs=[vm],
        out_specs=(vm, vm, vm),
        scratch_shapes=[pltpu.VMEM((m, n * hb, LANES), F32)],
        name='lists',
    )(ids)


def barrier(n, me):
    sem = pltpu.get_barrier_semaphore()
    for k in range(1, n):
        pl.semaphore_signal(sem, inc=1, device_id={'tp': lax.rem(me + k, n)}, device_id_type=MESH)
    pl.semaphore_wait(sem, n - 1)


def core_kernel(n, rows_ref, code_ref, tgt_ref, gain_ref, dy_hbm, y_hbm, sums_hbm, dg_ref,
                got, relay, dy, y, dx, xs, psend, prelay, dgacc, dgs,
                fsend, frecv, bsend, brecv, tsend, trecv, gsend, grecv, local):
    m = n // CORES
    tokens, hidden = dy_hbm.shape
    tile, sub = 128, 16
    tiles = tokens // tile
    me = lax.axis_index('tp')
    chip, core = me // CORES, lax.rem(me, CORES)
    step = 1 - 2 * core
    ahead, behind, far = (lax.rem(chip + step + m, m), lax.rem(chip - step + m, m), lax.rem(chip + 2, m))
    sib = chip * CORES + 1 - core

    def dev(c):
        return c * CORES + core

    def remote(src, dst, s, r, d):
        return pltpu.make_async_remote_copy(
            src_ref=src, dst_ref=dst, send_sem=s, recv_sem=r, device_id={'tp': d}, device_id_type=MESH)

    def slot(d):
        return got.at[pl.ds(pl.multiple_of(d * CAP, CAP), CAP)]

    dy_in = pltpu.make_async_copy(dy_hbm, dy, local.at[0])
    dy_in.start()
    own = pltpu.make_async_copy(rows_ref.at[chip], slot(me), local.at[1])
    own.start()
    barrier(n, me)

    to_far = remote(rows_ref.at[far], relay, fsend.at[0], frecv.at[n], dev(ahead))
    to_far.start()
    to_behind = remote(rows_ref.at[behind], slot(me), fsend.at[2], frecv.at[me], dev(behind))
    to_behind.start()
    to_ahead = remote(rows_ref.at[ahead], slot(me), fsend.at[1], frecv.at[me], dev(ahead))
    to_ahead.start()
    to_sib = remote(rows_ref.at[chip], slot(me), fsend.at[3], frecv.at[me], sib)
    to_sib.start()
    to_far.wait_recv()
    passed = remote(relay, slot(dev(behind)), fsend.at[4], frecv.at[dev(behind)], dev(ahead))
    passed.start()
    shared = []
    for k, source in enumerate((ahead, behind, far)):
        d = dev(source)
        share = remote(slot(d), slot(d), fsend.at[5 + k], frecv.at[d], sib)
        share.wait_recv()
        share.start()
        shared.append(share)
    for source in (chip, ahead, behind, far):
        d = source * CORES + 1 - core
        remote(slot(d), slot(d), fsend.at[3], frecv.at[d], sib).wait_recv()
    own.wait()
    dy_in.wait()

    dgacc[...] = jnp.zeros_like(dgacc)
    gain = gain_ref[...].astype(F32)

    def mine(t):
        return dx.at[pl.ds(pl.multiple_of(core * tokens + t * tile, tile), tile)]

    def swap(t):
        return remote(mine(t), mine(t), tsend.at[t], trecv.at[t], sib)

    def y_out(t):
        where = pl.ds(pl.multiple_of(t * tile, tile), tile)
        return pltpu.make_async_copy(y.at[where], y_hbm.at[where], local.at[2])

    def norm_tile(t, carry):
        at = pl.multiple_of(core * tokens + t * tile, tile)
        codes = jnp.broadcast_to(code_ref[:, pl.ds(at, tile)], (LANES, tile)).T
        pick = jnp.concatenate(
            [onehot(codes == tgt_ref[:, k:k + LANES]) for k in range(0, tgt_ref.shape[1], LANES)], axis=1)
        xs[...] = jnp.dot(pick, got[...], preferred_element_type=F32)

        def piece(k, c):
            here = pl.ds(pl.multiple_of(k * sub, sub), sub)
            glob = pl.ds(pl.multiple_of(t * tile + k * sub, sub), sub)
            h = xs[here, :]
            r = lax.rsqrt(jnp.mean(h * h, axis=-1, keepdims=True) + RMS_EPS)
            xh = h * r
            y[glob, :] = (xh.astype(BF16).astype(F32) * gain).astype(BF16)
            g = dy[glob, :].astype(F32)
            part = g * xh
            dgacc[...] += part[:8] + part[8:]
            u = g * gain
            mean = jnp.mean(u * xh, axis=-1, keepdims=True)
            dx[pl.ds(pl.multiple_of(at + k * sub, sub), sub), :] = (r * (u - xh * mean)).astype(BF16)
            return c

        lax.fori_loop(0, tile // sub, piece, 0)
        swap(t).start()
        return carry

    lax.fori_loop(0, tiles, norm_tile, 0)
    y_copy = pltpu.make_async_copy(y, y_hbm, local.at[2])
    y_copy.start()

    dgs[me] = jnp.sum(dgacc[...], axis=0, keepdims=True)
    for k in range(1, n):
        remote(dgs.at[me], dgs.at[me], gsend.at[k], grecv.at[k], lax.rem(me + k, n)).start()

    def swapped(t, carry):
        swap(t).wait()
        return carry

    lax.fori_loop(0, tiles, swapped, 0)

    wide = 512
    place = lax.broadcasted_iota(jnp.int32, (CAP, CORES * tokens), 0)

    def sums(q, dest):
        pick = onehot((place + dev(dest) * CODE).astype(F32) == code_ref[...])

        def part(k, c):
            cols = pl.ds(pl.multiple_of(k * wide, wide), wide)
            psend[q, :, cols] = jnp.dot(pick, dx[:, cols], preferred_element_type=F32)
            return c

        lax.fori_loop(0, hidden // wide, part, 0)

    sums(0, far)
    back_far = remote(psend.at[0], prelay, bsend.at[0], brecv.at[m], dev(ahead))
    back_far.start()
    sums(1, behind)
    back_behind = remote(psend.at[1], sums_hbm.at[chip], bsend.at[1], brecv.at[chip], dev(behind))
    back_behind.start()
    sums(2, ahead)
    back_ahead = remote(psend.at[2], sums_hbm.at[chip], bsend.at[2], brecv.at[chip], dev(ahead))
    back_ahead.start()
    sums(3, chip)
    keep = pltpu.make_async_copy(psend.at[3], sums_hbm.at[chip], local.at[3])
    keep.start()
    back_far.wait_recv()
    back_pass = remote(prelay, sums_hbm.at[behind], bsend.at[3], brecv.at[behind], dev(ahead))
    back_pass.start()

    for k in range(1, n):
        remote(dgs.at[me], dgs.at[lax.rem(me - k + n, n)], gsend.at[k], grecv.at[k], sib).wait()
    total = dgs[0]
    for k in range(1, n):
        total = total + dgs[k]
    dg_ref[...] = total

    for k, source in enumerate((ahead, behind, far)):
        remote(psend.at[0], sums_hbm.at[source], bsend.at[0], brecv.at[source], sib).wait_recv()
    for copy in (to_far, to_behind, to_ahead, to_sib, passed, *shared, back_far, back_behind, back_ahead, back_pass):
        copy.wait_send()
    keep.wait()
    y_copy.wait()


def short_path(n, table, uid, code, gain, grad):
    m = n // CORES
    _, tokens, hidden = grad.shape
    take = uid[:, 0]
    send = jnp.take(table, take, axis=0, mode='clip').reshape(m, CAP, hidden)
    k = jnp.arange(n * CAP)
    tgt = ((k // CAP) * CODE + k % CAP).astype(F32)[None]
    vm = pl.BlockSpec(memory_space=pltpu.VMEM)
    hbm = pl.BlockSpec(memory_space=pl.ANY)
    dma = pltpu.SemaphoreType.DMA
    tiles = tokens // 128
    y, sums, dg = pl.pallas_call(
        functools.partial(core_kernel, n),
        out_shape=(
            jax.ShapeDtypeStruct((tokens, hidden), BF16),
            jax.ShapeDtypeStruct((m, CAP, hidden), F32),
            jax.ShapeDtypeStruct((1, hidden), F32),
        ),
        in_specs=[vm, vm, vm, vm, hbm],
        out_specs=(hbm, hbm, vm),
        scratch_shapes=[
            pltpu.VMEM((n * CAP, hidden), BF16),
            pltpu.VMEM((CAP, hidden), BF16),
            pltpu.VMEM((tokens, hidden), BF16),
            pltpu.VMEM((tokens, hidden), BF16),
            pltpu.VMEM((CORES * tokens, hidden), BF16),
            pltpu.VMEM((128, hidden), F32),
            pltpu.VMEM((m, CAP, hidden), F32),
            pltpu.VMEM((CAP, hidden), F32),
            pltpu.VMEM((8, hidden), F32),
            pltpu.VMEM((n, 1, hidden), F32),
            dma((8,)), dma((n + 1,)), dma((m,)), dma((m + 1,)), dma((tiles,)), dma((tiles,)), dma((n,)), dma((n,)),
            dma((4,)),
        ],
        compiler_params=pltpu.CompilerParams(
            collective_id=0, has_side_effects=True, vmem_limit_bytes=60 * 1024 * 1024),
        name='short_path',
    )(send, code, tgt, gain.reshape(1, hidden), grad[0])
    table_grad = jnp.zeros((table.shape[0], hidden), F32).at[take].add(sums.reshape(m * CAP, hidden), mode='drop')
    return y[None], table_grad, dg[0]


def exchange_kernel(n, per_dest, src, out, send, recv, local):
    me = lax.axis_index('tp')

    def block(d):
        return src.at[d] if per_dest else src

    barrier(n, me)
    own = pltpu.make_async_copy(block(me), out.at[me], local)
    own.start()
    copies = []
    for k in range(1, n):
        peer = lax.rem(me + k, n)
        copies.append(pltpu.make_async_remote_copy(
            src_ref=block(peer), dst_ref=out.at[me], send_sem=send.at[k], recv_sem=recv.at[k],
            device_id={'tp': peer}, device_id_type=MESH))
        copies[-1].start()
    own.wait()
    for copy in copies:
        copy.wait()


def exchange(n, src, collective_id, per_dest):
    shape = src.shape[1:] if per_dest else src.shape
    hbm = pl.BlockSpec(memory_space=pl.ANY)
    dma = pltpu.SemaphoreType.DMA
    return pl.pallas_call(
        functools.partial(exchange_kernel, n, per_dest),
        out_shape=jax.ShapeDtypeStruct((n, *shape), src.dtype),
        in_specs=[hbm],
        out_specs=hbm,
        scratch_shapes=[dma((n,)), dma((n,)), dma(())],
        compiler_params=pltpu.CompilerParams(collective_id=collective_id, has_side_effects=True),
        name=f'exchange{collective_id}',
    )(src)


def norm_pass(embedded, norm_gain, grad_block):
    hidden_f32 = embedded.astype(F32)
    inv_rms = lax.rsqrt(jnp.mean(hidden_f32 * hidden_f32, axis=-1, keepdims=True) + RMS_EPS)
    x_hat = hidden_f32 * inv_rms
    normed = x_hat.astype(BF16) * norm_gain
    grad_f32 = grad_block.astype(F32)
    gain_part = jnp.sum(grad_f32 * x_hat, axis=(0, 1))
    grad_hat = grad_f32 * norm_gain.astype(F32)
    grad_in = (inv_rms * (grad_hat - x_hat * jnp.mean(grad_hat * x_hat, axis=-1, keepdims=True))).astype(BF16)
    return normed, grad_in, gain_part


def dense_path(n, token_ids, table, gain, grad):
    rows, hidden = table.shape
    tokens = grad.shape[1]
    local_ids = token_ids.reshape(-1) - lax.axis_index('tp') * rows
    owned = (local_ids >= 0) & (local_ids < rows)
    looked_up = jnp.take(table, jnp.where(owned, local_ids, 0), axis=0)
    partial = jnp.where(owned[:, None], looked_up, jnp.zeros((), BF16)).reshape(n, tokens, hidden)
    embedded = jnp.sum(exchange(n, partial, 1, True).astype(F32), axis=0).astype(BF16)
    normed, grad_in, gain_part = norm_pass(embedded[None], gain, grad)
    grad_gain = jnp.sum(exchange(n, gain_part.reshape(-1, LANES), 2, False), axis=0).reshape(-1)
    grad_all = exchange(n, grad_in[0], 3, False).reshape(-1, hidden)
    segments = jnp.where(owned, local_ids, rows)
    table_grad = jax.ops.segment_sum(grad_all.astype(F32), segments, num_segments=rows)
    return normed, table_grad, grad_gain


def device_step(n, token_ids, table, gain, grad):
    uid, code, top = make_lists(token_ids, n, table.shape[0])
    fits = top[0, 0] < CAP
    return lax.cond(
        fits,
        lambda: short_path(n, table, uid, code, gain, grad),
        lambda: dense_path(n, token_ids, table, gain, grad),
    )


def solution(mesh):
    n = mesh.shape['tp']
    return jax.shard_map(
        functools.partial(device_step, n), mesh=mesh,
        in_specs=(P('dp', None), P('tp', None), P(None), P('dp', 'tp', None)),
        out_specs=(P('dp', 'tp', None), P(('dp', 'tp'), None), P('dp')), check_vma=False)
```

```python
import functools

import jax
import jax.numpy as jnp
from jax import lax
from jax.experimental import pallas as pl
from jax.experimental.pallas import tpu as pltpu
from jax.sharding import PartitionSpec as P

RMS_EPS = 1e-5
MESH = pl.DeviceIdType.MESH
LANES = 128
CORES = 2
CAP = 112
MULTI = 56
SINGLE = 72
UNION = 240
CODE = 256
STRIDE = 128
PARTS = 4
TILE = 128
BF16_MAX = 3.3895313892515355e38
NT = (((1,), (1,)), ((), ()))
TN = (((0,), (0,)), ((), ()))
F32, BF16 = jnp.float32, jnp.bfloat16


def onehot(mask):
    return jnp.where(mask, 1.0, 0.0).astype(BF16)


def lists_kernel(n, rows, ids_ref, table_hbm, uid_ref, kmap_ref, code_ref, send_ref, fits_ref,
                 table, picked, rank_f, rank_b, rank_u, uid_s, sem):
    m = n // CORES
    width = ids_ref.shape[1] // m
    hb = -(-rows // LANES)
    high = n * hb
    me = lax.axis_index('tp')
    chip = me // CORES
    table_in = pltpu.make_async_copy(table_hbm, table, sem.at[0])
    table_in.start()
    picked[...] = jnp.zeros_like(picked)

    def split(ids):
        owner = jnp.zeros_like(ids)
        for k in range(1, n):
            owner += (ids >= k * rows).astype(jnp.int32)
        local = ids - owner * rows
        return owner, owner * hb + (local >> 7), local & (LANES - 1)

    def hots(hi, lo):
        h = onehot(lax.broadcasted_iota(jnp.int32, (high, width), 0) == hi)
        l = onehot(lax.broadcasted_iota(jnp.int32, (LANES, width), 0) == lo)
        return h, l

    a = lax.broadcasted_iota(jnp.int32, (LANES, LANES), 0)
    b = lax.broadcasted_iota(jnp.int32, (LANES, LANES), 1)
    lower, ones = onehot(a < b), jnp.ones((LANES, LANES), BF16)
    ra = lax.broadcasted_iota(jnp.int32, (high, high), 0)
    rb = lax.broadcasted_iota(jnp.int32, (high, high), 1)
    first = jnp.zeros_like(ra)
    for k in range(1, n):
        first += jnp.where(ra >= k * hb, hb, 0)
    before = onehot((rb < ra) & (rb >= first))

    def ahead_of(mask):
        present = onehot(mask)
        inside = jnp.dot(present, lower, preferred_element_type=F32)
        total = jnp.dot(present, ones, preferred_element_type=F32).astype(BF16)
        return inside + jnp.dot(before, total, preferred_element_type=F32)

    def over(mask, rank, cap):
        return jnp.where(mask & (rank > cap - 0.5), 1.0, 0.0)

    union = jnp.zeros((high, LANES), F32)
    bad = jnp.zeros((high, LANES), F32)
    for j in range(m):
        _, hi, lo = split(ids_ref[:, j * width:(j + 1) * width])
        h, l = hots(hi, lo)
        count = lax.dot_general(h, l, NT, preferred_element_type=F32)
        union += count
        here, many = count > 0.5, count > 1.5
        all_before, many_before = ahead_of(here), ahead_of(many)
        one_before = all_before - many_before
        bad += over(here, all_before, CAP) + over(many, many_before, MULTI) + over(count == 1.0, one_before, SINGLE)
        back = jnp.where(many, many_before, one_before + MULTI)
        rank_f[j] = jnp.where(here, jnp.minimum(all_before, CODE - 1.0), -1.0)
        rank_b[j] = jnp.where(here, jnp.minimum(back, CODE - 1.0), -1.0)
    here = union > 0.5
    all_before = ahead_of(here)
    bad += over(here, all_before, UNION)
    rank_u[...] = jnp.where(here, jnp.minimum(all_before, CODE - 1.0), -1.0)
    fits_ref[0, 0] = (jnp.max(bad) < 0.5).astype(jnp.int32)

    block = pl.ds(pl.multiple_of(me * hb, hb), hb)
    of_union = rank_u[block, :]
    lane = lax.broadcasted_iota(jnp.int32, (1, LANES), 1)
    every = jnp.ones((8, LANES), F32)

    def places(height):
        return lax.broadcasted_iota(jnp.int32, (height, LANES), 0).astype(F32)

    def as_row(found):
        return lax.dot_general(every, found, NT, preferred_element_type=F32, precision=lax.Precision.HIGHEST)[:1, :]

    want = places(CODE)
    found = jnp.zeros((CODE, LANES), F32)
    for k in range(hb):
        found += jnp.where(of_union[k:k + 1, :] == want, (k * LANES + lane).astype(F32), 0.0)
    length = jnp.max(of_union) + 1.0
    place = lax.broadcasted_iota(jnp.int32, (1, CODE), 1).astype(F32)
    uid_ref[...] = jnp.full(uid_ref.shape, rows, jnp.int32)
    uid_ref[:1, :] = jnp.where((place < length) & (place < UNION), as_row(found), float(rows)).astype(jnp.int32)
    uid_in = pltpu.make_async_copy(uid_ref, uid_s, sem.at[1])
    uid_in.start()

    owner, hi, lo = split(ids_ref[:, pl.ds(pl.multiple_of(chip * width, width), width)])
    h, l = hots(hi, lo)
    l = l.astype(F32)
    for k, rank in enumerate((rank_f, rank_b)):
        found = lax.dot_general(rank[chip].astype(BF16), h, TN, preferred_element_type=F32)
        code_ref[k:k + 1, :] = owner.astype(F32) * CODE + jnp.sum(found * l, axis=0, keepdims=True)

    want = places(LANES)
    spread = []
    for j in range(m):
        fwd, back = rank_f[j, block, :], rank_b[j, block, :]
        found_f = jnp.zeros((CAP, LANES), F32)
        found_b = jnp.zeros((LANES, LANES), F32)
        for k in range(hb):
            u = of_union[k:k + 1, :]
            found_f += jnp.where(fwd[k:k + 1, :] == want[:CAP], u, 0.0)
            found_b += jnp.where(back[k:k + 1, :] == want, u + 1.0, 0.0)
        of_slot = jnp.sum(found_f, axis=1, keepdims=True)
        spread.append(onehot(lax.broadcasted_iota(jnp.int32, (CAP, CODE), 1).astype(F32) == of_slot))
        row = as_row(found_b) - 1.0
        again = jnp.where(lane < MULTI, row, jnp.where(lane < 2 * MULTI, pltpu.roll(row, MULTI, 1), -1.0))
        kmap_ref[j:j + 1, :] = jnp.concatenate([row, again], axis=1)

    uid_in.wait()
    table_in.wait()
    pack, eight = 16, 8
    sublane = lax.broadcasted_iota(jnp.int32, (eight, table.shape[2]), 0)
    groups = jnp.minimum((length.astype(jnp.int32) + pack - 1) // pack, UNION // pack)

    def pick(q, carry):
        halves = []
        for half in range(pack // eight):
            acc = jnp.zeros(sublane.shape, F32)
            for k in range(eight):
                v = jnp.minimum(uid_s[0, q * pack + half * eight + k], rows - 1)
                tile = table[v // eight].astype(F32)
                turned = pltpu.roll(tile, lax.rem(k + eight - lax.rem(v, eight), eight), 0)
                acc = jnp.where(sublane == k, turned, acc)
            halves.append(acc)
        picked[pl.ds(pl.multiple_of(q * pack, pack), pack), :] = jnp.concatenate(halves, axis=0).astype(BF16)
        return carry

    lax.fori_loop(0, groups, pick, 0)
    for j in range(m):
        send_ref[j] = jnp.dot(spread[j], picked[...], preferred_element_type=F32).astype(BF16)


def make_lists(token_ids, table, n):
    m = n // CORES
    rows, hidden = table.shape
    hb = -(-rows // LANES)
    vm = pl.BlockSpec(memory_space=pltpu.VMEM)
    return pl.pallas_call(
        functools.partial(lists_kernel, n, rows),
        out_shape=(
            jax.ShapeDtypeStruct((8, CODE), jnp.int32),
            jax.ShapeDtypeStruct((m, 2 * LANES), F32),
            jax.ShapeDtypeStruct((2, token_ids.shape[1] // m), F32),
            jax.ShapeDtypeStruct((m, CAP, hidden), BF16),
            jax.ShapeDtypeStruct((1, 1), jnp.int32),
        ),
        in_specs=[vm, pl.BlockSpec(memory_space=pl.ANY)],
        out_specs=(vm, vm, vm, vm, pl.BlockSpec(memory_space=pltpu.SMEM)),
        scratch_shapes=[
            pltpu.VMEM((rows // 8, 8, hidden), BF16),
            pltpu.VMEM((CODE, hidden), BF16),
            pltpu.VMEM((m, n * hb, LANES), F32),
            pltpu.VMEM((m, n * hb, LANES), F32),
            pltpu.VMEM((n * hb, LANES), F32),
            pltpu.SMEM((8, CODE), jnp.int32),
            pltpu.SemaphoreType.DMA((2,)),
        ],
        compiler_params=pltpu.CompilerParams(vmem_limit_bytes=44 * 1024 * 1024),
        name='lists',
    )(token_ids, table.reshape(rows // 8, 8, hidden))


def barrier(n, me):
    sem = pltpu.get_barrier_semaphore()
    for k in range(1, n):
        pl.semaphore_signal(sem, inc=1, device_id={'tp': lax.rem(me + k, n)}, device_id_type=MESH)
    pl.semaphore_wait(sem, n - 1)


def core_kernel(n, rows_ref, code_ref, kmap_ref, gain_ref, dy_hbm, y, merged, dg_ref,
                got, relay, dy, dx, xs, codes, pick_x, psum, pone, rsum, rone, gsum, gone, dgacc, dgs,
                fsend, frecv, bsend, brecv, psend, precv, tsend, trecv, gsend, grecv, local):
    m = n // CORES
    tokens, hidden = dy_hbm.shape
    tiles = tokens // TILE
    me = lax.axis_index('tp')
    chip, core = me // CORES, lax.rem(me, CORES)
    step = 1 - 2 * core
    ahead, behind, far = (lax.rem(chip + step + m, m), lax.rem(chip - step + m, m), lax.rem(chip + 2, m))
    sib = chip * CORES + 1 - core

    def dev(c):
        return c * CORES + core

    def remote(src, dst, s, r, d):
        return pltpu.make_async_remote_copy(
            src_ref=src, dst_ref=dst, send_sem=s, recv_sem=r, device_id={'tp': d}, device_id_type=MESH)

    def slot(d):
        return got.at[pl.ds(pl.multiple_of(d * STRIDE, STRIDE), CAP)]

    dy_in = pltpu.make_async_copy(dy_hbm, dy, local.at[0])
    dy_in.start()
    own = pltpu.make_async_copy(rows_ref.at[chip], slot(me), local.at[1])
    own.start()
    barrier(n, me)

    to_far = remote(rows_ref.at[far], relay, fsend.at[0], frecv.at[n], dev(ahead))
    to_far.start()
    to_behind = remote(rows_ref.at[behind], slot(me), fsend.at[2], frecv.at[me], dev(behind))
    to_behind.start()
    to_ahead = remote(rows_ref.at[ahead], slot(me), fsend.at[1], frecv.at[me], dev(ahead))
    to_ahead.start()
    to_sib = remote(rows_ref.at[chip], slot(me), fsend.at[3], frecv.at[me], sib)
    to_sib.start()

    lane = lax.broadcasted_iota(jnp.int32, (1, LANES), 1).astype(F32)
    for d in range(n):
        got[d * STRIDE + CAP:(d + 1) * STRIDE, :] = jnp.zeros((STRIDE - CAP, hidden), BF16)
    dgacc[...] = jnp.zeros_like(dgacc)

    def turn(t, carry):
        at = pl.multiple_of(core * tokens + t * TILE, TILE)
        codes[pl.ds(pl.multiple_of(t * TILE, TILE), TILE), :] = jnp.broadcast_to(
            code_ref[:1, pl.ds(at, TILE)], (LANES, TILE)).T
        return carry

    lax.fori_loop(0, tiles, turn, 0)
    wide = hidden // PARTS

    def add_rows(source, init):
        for o in range(CORES):
            base = ((source * CORES + o) * CODE).astype(F32)
            pick_x[:, o * LANES:(o + 1) * LANES] = onehot(codes[...] == lane + base)
        rows = pl.ds(pl.multiple_of(source * CORES * STRIDE, CORES * STRIDE), CORES * STRIDE)

        def part(k, c):
            cols = pl.ds(pl.multiple_of(k * wide, wide), wide)
            term = jnp.dot(pick_x[...], got[rows, cols], preferred_element_type=F32)
            if init:
                xs[:, cols] = term
            else:
                xs[:, cols] += term
            return c

        lax.fori_loop(0, hidden // wide, part, 0)

    def from_sib(source):
        d = source * CORES + 1 - core
        remote(slot(d), slot(d), fsend.at[3], frecv.at[d], sib).wait_recv()

    shared = []

    def share(k, source):
        d = dev(source)
        copy = remote(slot(d), slot(d), fsend.at[5 + k], frecv.at[d], sib)
        copy.wait_recv()
        copy.start()
        shared.append(copy)

    own.wait()
    from_sib(chip)
    add_rows(chip, True)
    to_far.wait_recv()
    passed = remote(relay, slot(dev(behind)), fsend.at[4], frecv.at[dev(behind)], dev(ahead))
    passed.start()
    share(0, ahead)
    share(1, behind)
    for source in (behind, ahead):
        from_sib(source)
        add_rows(source, False)
    share(2, far)
    from_sib(far)
    add_rows(far, False)
    dy_in.wait()

    gain = gain_ref[...].astype(F32).reshape(1, hidden)
    columns = range(0, hidden, LANES)

    def mine(t):
        return dx.at[pl.ds(pl.multiple_of(core * tokens + t * TILE, TILE), TILE)]

    def swap(t):
        return remote(mine(t), mine(t), tsend.at[t], trecv.at[t], sib)

    def norm_tile(t, carry):
        here = pl.ds(pl.multiple_of(t * TILE, TILE), TILE)
        there = pl.ds(pl.multiple_of(core * tokens + t * TILE, TILE), TILE)
        acc = jnp.zeros((TILE, LANES), F32)
        for c in columns:
            h = xs[here, c:c + LANES]
            acc += h * h
        r = lax.rsqrt(jnp.sum(acc, axis=-1, keepdims=True) / hidden + RMS_EPS)
        r = jnp.broadcast_to(r, (TILE, LANES))
        acc = jnp.zeros((TILE, LANES), F32)
        for c in columns:
            xh = xs[here, c:c + LANES] * r
            gain_c = gain[:, c:c + LANES]
            y[here, c:c + LANES] = (xh.astype(BF16).astype(F32) * gain_c).astype(BF16)
            g = dy[here, c:c + LANES].astype(F32)
            part = g * xh
            acc += g * gain_c * xh
            dgacc[:, c:c + LANES] += jnp.sum(part.reshape(TILE // 8, 8, LANES), axis=0)
        mean = jnp.broadcast_to(jnp.sum(acc, axis=-1, keepdims=True) / hidden, (TILE, LANES))
        for c in columns:
            xh = xs[here, c:c + LANES] * r
            u = dy[here, c:c + LANES].astype(F32) * gain[:, c:c + LANES]
            dx[there, c:c + LANES] = (r * (u - xh * mean)).astype(BF16)
        swap(t).start()
        return carry

    lax.fori_loop(0, tiles, norm_tile, 0)

    dgs[me] = jnp.sum(dgacc[...], axis=0, keepdims=True)
    for k in range(1, n):
        remote(dgs.at[me], dgs.at[me], gsend.at[k], grecv.at[k], lax.rem(me + k, n)).start()

    def swapped(t, carry):
        swap(t).wait()
        return carry

    lax.fori_loop(0, tiles, swapped, 0)

    place = lax.broadcasted_iota(jnp.int32, (LANES, CORES * tokens), 0)

    def picks(dest):
        return onehot((place + dev(dest) * CODE).astype(F32) == code_ref[1:2, :])

    def sums(q, pick, k):
        cols = pl.ds(pl.multiple_of(k * wide, wide), wide)
        total = jnp.dot(pick, dx[:, cols], preferred_element_type=F32)
        psum[q, k] = total[:MULTI]
        pone[q, k] = total[MULTI:].astype(BF16)

    def all_sums(q, dest):
        pick = picks(dest)

        def part(k, c):
            sums(q, pick, k)
            return c

        lax.fori_loop(0, PARTS, part, 0)

    first, relays = [], []
    pick = picks(far)
    for k in range(PARTS):
        sums(0, pick, k)
        for w, (mine_, relay_) in enumerate(((psum, rsum), (pone, rone))):
            first.append(remote(mine_.at[0, k], relay_.at[k], psend.at[w, 0, k], precv.at[w, 0, k], dev(ahead)))
            first[-1].start()

    def back(q, dest, sem):
        out = []
        for w, (mine_, theirs) in enumerate(((psum, gsum), (pone, gone))):
            out.append(remote(mine_.at[q], theirs.at[chip], bsend.at[w, sem], brecv.at[w, chip], dev(dest)))
            out[-1].start()
        return out

    all_sums(1, behind)
    direct = back(1, behind, 0)
    all_sums(2, ahead)
    direct += back(2, ahead, 1)
    all_sums(3, chip)

    def merge(source, multi, single, init):
        index = kmap_ref[pl.ds(source, 1), :]
        pick = onehot(lax.broadcasted_iota(jnp.int32, (UNION, 2 * LANES), 0).astype(F32) == index)
        pad = jnp.zeros((2 * LANES - 3 * MULTI - SINGLE, wide), F32)

        def part(k, c):
            cols = pl.ds(pl.multiple_of(k * wide, wide), wide)
            p = multi[k]
            high = jnp.clip(p, -BF16_MAX, BF16_MAX).astype(BF16).astype(F32)
            rest = p - high
            mid = rest.astype(BF16).astype(F32)
            stack = jnp.concatenate([high, single[k].astype(F32), mid, rest - mid, pad], axis=0).astype(BF16)
            term = jnp.dot(pick, stack, preferred_element_type=F32)
            if init:
                merged[:, cols] = term
            else:
                merged[:, cols] += term
            return c

        lax.fori_loop(0, PARTS, part, 0)

    for k in range(PARTS):
        for w, (relay_, theirs) in enumerate(((rsum, gsum), (rone, gone))):
            first[2 * k + w].wait_recv()
            relays.append(remote(relay_.at[k], theirs.at[behind, k], psend.at[w, 1, k], precv.at[w, 1, k], dev(ahead)))
            relays[-1].start()
    merge(chip, psum.at[3], pone.at[3], True)

    for k in range(1, n):
        remote(dgs.at[me], dgs.at[lax.rem(me - k + n, n)], gsend.at[k], grecv.at[k], sib).wait()
    total = dgs[0]
    for k in range(1, n):
        total = total + dgs[k]
    dg_ref[...] = total

    for source in (ahead, behind):
        for w, (mine_, theirs) in enumerate(((psum, gsum), (pone, gone))):
            remote(mine_.at[0], theirs.at[source], bsend.at[w, 0], brecv.at[w, source], sib).wait_recv()
        merge(source, gsum.at[source], gone.at[source], False)
    for copy in relays:
        copy.wait_recv()
    merge(far, gsum.at[far], gone.at[far], False)
    for copy in (to_far, to_behind, to_ahead, to_sib, passed, *shared, *first, *direct, *relays):
        copy.wait_send()


def write_kernel(uid_s, merged_ref, y_ref, dg_ref, table_grad_ref, y_out, dg_out, at, sem):
    step, tile = pl.program_id(0), table_grad_ref.shape[0]
    y_copy = pltpu.make_async_copy(y_ref, y_out, sem.at[0])

    @pl.when(step == 0)
    def _():
        y_copy.start()
        dg_out[...] = dg_ref[...]
        at[0] = 0

    table_grad_ref[...] = jnp.zeros_like(table_grad_ref)

    def more(p):
        return uid_s[0, p] < (step + 1) * tile

    def put(p):
        table_grad_ref[pl.ds(uid_s[0, p] - step * tile, 1), :] = merged_ref[pl.ds(p, 1), :]
        return p + 1

    at[0] = lax.while_loop(more, put, at[0])

    @pl.when(step == pl.num_programs(0) - 1)
    def _():
        y_copy.wait()


def write_out(rows, uid, merged, y, dg):
    tokens, hidden = y.shape
    tile = next(t for t in range(160, 0, -8) if rows % t == 0)
    hbm = pl.BlockSpec(memory_space=pl.ANY)
    vm = pl.BlockSpec(memory_space=pltpu.VMEM)
    return pl.pallas_call(
        write_kernel,
        grid=(rows // tile,),
        out_shape=(
            jax.ShapeDtypeStruct((rows, hidden), F32),
            jax.ShapeDtypeStruct((tokens, hidden), BF16),
            jax.ShapeDtypeStruct((1, hidden), F32),
        ),
        in_specs=[pl.BlockSpec(memory_space=pltpu.SMEM), vm, vm, vm],
        out_specs=(pl.BlockSpec((tile, hidden), lambda i: (i, 0)), hbm, vm),
        scratch_shapes=[pltpu.SMEM((1,), jnp.int32), pltpu.SemaphoreType.DMA((1,))],
        compiler_params=pltpu.CompilerParams(vmem_limit_bytes=24 * 1024 * 1024),
        name='write_out',
    )(uid, merged, y, dg)


def short_path(n, rows, uid, kmap, code, send, gain, grad):
    m = n // CORES
    _, tokens, hidden = grad.shape
    vm = pl.BlockSpec(memory_space=pltpu.VMEM)
    hbm = pl.BlockSpec(memory_space=pl.ANY)
    dma = pltpu.SemaphoreType.DMA
    tiles = tokens // TILE
    y, merged, dg = pl.pallas_call(
        functools.partial(core_kernel, n),
        out_shape=(
            jax.ShapeDtypeStruct((tokens, hidden), BF16),
            jax.ShapeDtypeStruct((UNION, hidden), F32),
            jax.ShapeDtypeStruct((1, hidden), F32),
        ),
        in_specs=[vm, vm, vm, vm, hbm],
        out_specs=(vm, vm, vm),
        scratch_shapes=[
            pltpu.VMEM((n * STRIDE, hidden), BF16),
            pltpu.VMEM((CAP, hidden), BF16),
            pltpu.VMEM((tokens, hidden), BF16),
            pltpu.VMEM((CORES * tokens, hidden), BF16),
            pltpu.VMEM((tokens, hidden), F32),
            pltpu.VMEM((tokens, LANES), F32),
            pltpu.VMEM((tokens, CORES * LANES), BF16),
            pltpu.VMEM((m, PARTS, MULTI, hidden // PARTS), F32),
            pltpu.VMEM((m, PARTS, SINGLE, hidden // PARTS), BF16),
            pltpu.VMEM((PARTS, MULTI, hidden // PARTS), F32),
            pltpu.VMEM((PARTS, SINGLE, hidden // PARTS), BF16),
            pltpu.VMEM((m, PARTS, MULTI, hidden // PARTS), F32),
            pltpu.VMEM((m, PARTS, SINGLE, hidden // PARTS), BF16),
            pltpu.VMEM((8, hidden), F32),
            pltpu.VMEM((n, 1, hidden), F32),
            dma((8,)), dma((n + 1,)), dma((2, 2)), dma((2, m)), dma((2, 2, PARTS)), dma((2, 2, PARTS)),
            dma((tiles,)), dma((tiles,)), dma((n,)), dma((n,)), dma((2,)),
        ],
        compiler_params=pltpu.CompilerParams(
            collective_id=0, has_side_effects=True, vmem_limit_bytes=52 * 1024 * 1024),
        name='short_path',
    )(send, code, kmap, gain, grad[0])
    table_grad, y, dg = write_out(rows, uid, merged, y, dg)
    return y[None], table_grad, dg[0]


def exchange_kernel(n, per_dest, src, out, send, recv, local):
    me = lax.axis_index('tp')

    def block(d):
        return src.at[d] if per_dest else src

    barrier(n, me)
    own = pltpu.make_async_copy(block(me), out.at[me], local)
    own.start()
    copies = []
    for k in range(1, n):
        peer = lax.rem(me + k, n)
        copies.append(pltpu.make_async_remote_copy(
            src_ref=block(peer), dst_ref=out.at[me], send_sem=send.at[k], recv_sem=recv.at[k],
            device_id={'tp': peer}, device_id_type=MESH))
        copies[-1].start()
    own.wait()
    for copy in copies:
        copy.wait()


def exchange(n, src, collective_id, per_dest):
    shape = src.shape[1:] if per_dest else src.shape
    hbm = pl.BlockSpec(memory_space=pl.ANY)
    dma = pltpu.SemaphoreType.DMA
    return pl.pallas_call(
        functools.partial(exchange_kernel, n, per_dest),
        out_shape=jax.ShapeDtypeStruct((n, *shape), src.dtype),
        in_specs=[hbm],
        out_specs=hbm,
        scratch_shapes=[dma((n,)), dma((n,)), dma(())],
        compiler_params=pltpu.CompilerParams(collective_id=collective_id, has_side_effects=True),
        name=f'exchange{collective_id}',
    )(src)


def norm_pass(embedded, norm_gain, grad_block):
    hidden_f32 = embedded.astype(F32)
    inv_rms = lax.rsqrt(jnp.mean(hidden_f32 * hidden_f32, axis=-1, keepdims=True) + RMS_EPS)
    x_hat = hidden_f32 * inv_rms
    normed = x_hat.astype(BF16) * norm_gain
    grad_f32 = grad_block.astype(F32)
    gain_part = jnp.sum(grad_f32 * x_hat, axis=(0, 1))
    grad_hat = grad_f32 * norm_gain.astype(F32)
    grad_in = (inv_rms * (grad_hat - x_hat * jnp.mean(grad_hat * x_hat, axis=-1, keepdims=True))).astype(BF16)
    return normed, grad_in, gain_part


def dense_path(n, token_ids, table, gain, grad):
    rows, hidden = table.shape
    tokens = grad.shape[1]
    local_ids = token_ids.reshape(-1) - lax.axis_index('tp') * rows
    owned = (local_ids >= 0) & (local_ids < rows)
    looked_up = jnp.take(table, jnp.where(owned, local_ids, 0), axis=0)
    partial = jnp.where(owned[:, None], looked_up, jnp.zeros((), BF16)).reshape(n, tokens, hidden)
    embedded = jnp.sum(exchange(n, partial, 1, True).astype(F32), axis=0).astype(BF16)
    normed, grad_in, gain_part = norm_pass(embedded[None], gain, grad)
    grad_gain = jnp.sum(exchange(n, gain_part.reshape(-1, LANES), 2, False), axis=0).reshape(-1)
    grad_all = exchange(n, grad_in[0], 3, False).reshape(-1, hidden)
    segments = jnp.where(owned, local_ids, rows)
    table_grad = jax.ops.segment_sum(grad_all.astype(F32), segments, num_segments=rows)
    return normed, table_grad, grad_gain


def device_step(n, token_ids, table, gain, grad):
    uid, kmap, code, send, fits = make_lists(token_ids, table, n)
    return lax.cond(
        fits[0, 0] == 1,
        lambda: short_path(n, table.shape[0], uid, kmap, code, send, gain, grad),
        lambda: dense_path(n, token_ids, table, gain, grad),
    )


def solution(mesh):
    n = mesh.shape['tp']
    return jax.shard_map(
        functools.partial(device_step, n), mesh=mesh,
        in_specs=(P('dp', None), P('tp', None), P(None), P('dp', 'tp', None)),
        out_specs=(P('dp', 'tp', None), P(('dp', 'tp'), None), P('dp')), check_vma=False)
```

```python
import functools

import jax
import jax.numpy as jnp
from jax import lax
from jax.experimental import pallas as pl
from jax.experimental.pallas import tpu as pltpu
from jax.sharding import PartitionSpec as P

RMS_EPS = 1e-5
MESH = pl.DeviceIdType.MESH
LANES = 128
CORES = 2
CAP = 112
MULTI = 56
SINGLE = 72
UNION = 240
CODE = 256
STRIDE = 128
PARTS = 4
TILE = 128
BF16_MAX = 3.3895313892515355e38
NT = (((1,), (1,)), ((), ()))
TN = (((0,), (0,)), ((), ()))
F32, BF16 = jnp.float32, jnp.bfloat16


def onehot(mask):
    return jnp.where(mask, 1.0, 0.0).astype(BF16)


def lists_kernel(n, rows, ids_ref, table_hbm, uid_ref, kmap_ref, code_ref, send_ref, fits_ref,
                 table, picked, rank_f, rank_b, rank_u, uid_s, sem):
    m = n // CORES
    width = ids_ref.shape[1] // m
    hb = -(-rows // LANES)
    high = n * hb
    me = lax.axis_index('tp')
    chip = me // CORES
    table_in = pltpu.make_async_copy(table_hbm, table, sem.at[0])
    table_in.start()
    picked[...] = jnp.zeros_like(picked)

    def split(ids):
        owner = jnp.zeros_like(ids)
        for k in range(1, n):
            owner += (ids >= k * rows).astype(jnp.int32)
        local = ids - owner * rows
        return owner, owner * hb + (local >> 7), local & (LANES - 1)

    def hots(hi, lo):
        h = onehot(lax.broadcasted_iota(jnp.int32, (high, width), 0) == hi)
        l = onehot(lax.broadcasted_iota(jnp.int32, (LANES, width), 0) == lo)
        return h, l

    a = lax.broadcasted_iota(jnp.int32, (LANES, LANES), 0)
    b = lax.broadcasted_iota(jnp.int32, (LANES, LANES), 1)
    lower, ones = onehot(a < b), jnp.ones((LANES, LANES), BF16)
    ra = lax.broadcasted_iota(jnp.int32, (high, high), 0)
    rb = lax.broadcasted_iota(jnp.int32, (high, high), 1)
    first = jnp.zeros_like(ra)
    for k in range(1, n):
        first += jnp.where(ra >= k * hb, hb, 0)
    before = onehot((rb < ra) & (rb >= first))

    def ahead_of(mask):
        present = onehot(mask)
        inside = jnp.dot(present, lower, preferred_element_type=F32)
        total = jnp.dot(present, ones, preferred_element_type=F32).astype(BF16)
        return inside + jnp.dot(before, total, preferred_element_type=F32)

    def over(mask, rank, cap):
        return jnp.where(mask & (rank > cap - 0.5), 1.0, 0.0)

    union = jnp.zeros((high, LANES), F32)
    bad = jnp.zeros((high, LANES), F32)
    for j in range(m):
        _, hi, lo = split(ids_ref[:, j * width:(j + 1) * width])
        h, l = hots(hi, lo)
        count = lax.dot_general(h, l, NT, preferred_element_type=F32)
        union += count
        here, many = count > 0.5, count > 1.5
        all_before, many_before = ahead_of(here), ahead_of(many)
        one_before = all_before - many_before
        bad += over(here, all_before, CAP) + over(many, many_before, MULTI) + over(count == 1.0, one_before, SINGLE)
        back = jnp.where(many, many_before, one_before + MULTI)
        rank_f[j] = jnp.where(here, jnp.minimum(all_before, CODE - 1.0), -1.0)
        rank_b[j] = jnp.where(here, jnp.minimum(back, CODE - 1.0), -1.0)
    here = union > 0.5
    all_before = ahead_of(here)
    bad += over(here, all_before, UNION)
    rank_u[...] = jnp.where(here, jnp.minimum(all_before, CODE - 1.0), -1.0)
    fits_ref[0, 0] = (jnp.max(bad) < 0.5).astype(jnp.int32)

    block = pl.ds(pl.multiple_of(me * hb, hb), hb)
    of_union = rank_u[block, :]
    lane = lax.broadcasted_iota(jnp.int32, (1, LANES), 1)
    every = jnp.ones((8, LANES), F32)

    def places(height):
        return lax.broadcasted_iota(jnp.int32, (height, LANES), 0).astype(F32)

    def as_row(found):
        return lax.dot_general(every, found, NT, preferred_element_type=F32, precision=lax.Precision.HIGHEST)[:1, :]

    want = places(CODE)
    found = jnp.zeros((CODE, LANES), F32)
    for k in range(hb):
        found += jnp.where(of_union[k:k + 1, :] == want, (k * LANES + lane).astype(F32), 0.0)
    length = jnp.max(of_union) + 1.0
    place = lax.broadcasted_iota(jnp.int32, (1, CODE), 1).astype(F32)
    uid_ref[...] = jnp.full(uid_ref.shape, rows, jnp.int32)
    uid_ref[:1, :] = jnp.where((place < length) & (place < UNION), as_row(found), float(rows)).astype(jnp.int32)
    uid_in = pltpu.make_async_copy(uid_ref, uid_s, sem.at[1])
    uid_in.start()

    owner, hi, lo = split(ids_ref[:, pl.ds(pl.multiple_of(chip * width, width), width)])
    h, l = hots(hi, lo)
    l = l.astype(F32)
    for k, rank in enumerate((rank_f, rank_b)):
        found = lax.dot_general(rank[chip].astype(BF16), h, TN, preferred_element_type=F32)
        code_ref[k:k + 1, :] = owner.astype(F32) * CODE + jnp.sum(found * l, axis=0, keepdims=True)

    want = places(LANES)
    spread = []
    for j in range(m):
        fwd, back = rank_f[j, block, :], rank_b[j, block, :]
        found_f = jnp.zeros((CAP, LANES), F32)
        found_b = jnp.zeros((LANES, LANES), F32)
        for k in range(hb):
            u = of_union[k:k + 1, :]
            found_f += jnp.where(fwd[k:k + 1, :] == want[:CAP], u, 0.0)
            found_b += jnp.where(back[k:k + 1, :] == want, u + 1.0, 0.0)
        of_slot = jnp.sum(found_f, axis=1, keepdims=True)
        spread.append(onehot(lax.broadcasted_iota(jnp.int32, (CAP, CODE), 1).astype(F32) == of_slot))
        row = as_row(found_b) - 1.0
        again = jnp.where(lane < MULTI, row, jnp.where(lane < 2 * MULTI, pltpu.roll(row, MULTI, 1), -1.0))
        kmap_ref[j:j + 1, :] = jnp.concatenate([row, again], axis=1)

    uid_in.wait()
    table_in.wait()
    pack, eight = 16, 8
    sublane = lax.broadcasted_iota(jnp.int32, (eight, table.shape[2]), 0)
    groups = jnp.minimum((length.astype(jnp.int32) + pack - 1) // pack, UNION // pack)

    def pick(q, carry):
        halves = []
        for half in range(pack // eight):
            acc = jnp.zeros(sublane.shape, F32)
            for k in range(eight):
                v = jnp.minimum(uid_s[0, q * pack + half * eight + k], rows - 1)
                tile = table[v // eight].astype(F32)
                turned = pltpu.roll(tile, lax.rem(k + eight - lax.rem(v, eight), eight), 0)
                acc = jnp.where(sublane == k, turned, acc)
            halves.append(acc)
        picked[pl.ds(pl.multiple_of(q * pack, pack), pack), :] = jnp.concatenate(halves, axis=0).astype(BF16)
        return carry

    lax.fori_loop(0, groups, pick, 0)
    spread = jnp.concatenate(spread, axis=0)
    for c in range(0, table.shape[2], CODE):
        rows_out = jnp.dot(spread, picked[:, c:c + CODE], preferred_element_type=F32).astype(BF16)
        for j in range(m):
            send_ref[j, :, c:c + CODE] = rows_out[j * CAP:(j + 1) * CAP]


def make_lists(token_ids, table, n):
    m = n // CORES
    rows, hidden = table.shape
    hb = -(-rows // LANES)
    vm = pl.BlockSpec(memory_space=pltpu.VMEM)
    return pl.pallas_call(
        functools.partial(lists_kernel, n, rows),
        out_shape=(
            jax.ShapeDtypeStruct((8, CODE), jnp.int32),
            jax.ShapeDtypeStruct((m, 2 * LANES), F32),
            jax.ShapeDtypeStruct((2, token_ids.shape[1] // m), F32),
            jax.ShapeDtypeStruct((m, CAP, hidden), BF16),
            jax.ShapeDtypeStruct((1, 1), jnp.int32),
        ),
        in_specs=[vm, pl.BlockSpec(memory_space=pl.ANY)],
        out_specs=(vm, vm, vm, vm, pl.BlockSpec(memory_space=pltpu.SMEM)),
        scratch_shapes=[
            pltpu.VMEM((rows // 8, 8, hidden), BF16),
            pltpu.VMEM((CODE, hidden), BF16),
            pltpu.VMEM((m, n * hb, LANES), F32),
            pltpu.VMEM((m, n * hb, LANES), F32),
            pltpu.VMEM((n * hb, LANES), F32),
            pltpu.SMEM((8, CODE), jnp.int32),
            pltpu.SemaphoreType.DMA((2,)),
        ],
        compiler_params=pltpu.CompilerParams(vmem_limit_bytes=44 * 1024 * 1024),
        name='lists',
    )(token_ids, table.reshape(rows // 8, 8, hidden))


def barrier(n, me):
    sem = pltpu.get_barrier_semaphore()
    for k in range(1, n):
        pl.semaphore_signal(sem, inc=1, device_id={'tp': lax.rem(me + k, n)}, device_id_type=MESH)
    pl.semaphore_wait(sem, n - 1)


def core_kernel(n, rows_ref, code_ref, kmap_ref, gain_ref, dy_hbm, y_hbm, merged, dg_ref,
                got, relay, dy, y, dx, xs, codes, pick_x, psum, pone, rsum, rone, gsum, gone, dgacc, dgs,
                fsend, frecv, bsend, brecv, psend, precv, tsend, trecv, gsend, grecv, local):
    m = n // CORES
    tokens, hidden = dy_hbm.shape
    tiles = tokens // TILE
    me = lax.axis_index('tp')
    chip, core = me // CORES, lax.rem(me, CORES)
    step = 1 - 2 * core
    ahead, behind, far = (lax.rem(chip + step + m, m), lax.rem(chip - step + m, m), lax.rem(chip + 2, m))
    sib = chip * CORES + 1 - core

    def dev(c):
        return c * CORES + core

    def remote(src, dst, s, r, d):
        return pltpu.make_async_remote_copy(
            src_ref=src, dst_ref=dst, send_sem=s, recv_sem=r, device_id={'tp': d}, device_id_type=MESH)

    def slot(d):
        return got.at[pl.ds(pl.multiple_of(d * STRIDE, STRIDE), CAP)]

    dy_in = pltpu.make_async_copy(dy_hbm, dy, local.at[0])
    dy_in.start()
    own = pltpu.make_async_copy(rows_ref.at[chip], slot(me), local.at[1])
    own.start()
    barrier(n, me)

    to_far = remote(rows_ref.at[far], relay, fsend.at[0], frecv.at[n], dev(ahead))
    to_far.start()
    to_behind = remote(rows_ref.at[behind], slot(me), fsend.at[2], frecv.at[me], dev(behind))
    to_behind.start()
    to_ahead = remote(rows_ref.at[ahead], slot(me), fsend.at[1], frecv.at[me], dev(ahead))
    to_ahead.start()
    to_sib = remote(rows_ref.at[chip], slot(me), fsend.at[3], frecv.at[me], sib)
    to_sib.start()

    lane = lax.broadcasted_iota(jnp.int32, (1, LANES), 1).astype(F32)
    for d in range(n):
        got[d * STRIDE + CAP:(d + 1) * STRIDE, :] = jnp.zeros((STRIDE - CAP, hidden), BF16)
    dgacc[...] = jnp.zeros_like(dgacc)

    def turn(t, carry):
        at = pl.multiple_of(core * tokens + t * TILE, TILE)
        codes[pl.ds(pl.multiple_of(t * TILE, TILE), TILE), :] = jnp.broadcast_to(
            code_ref[:1, pl.ds(at, TILE)], (LANES, TILE)).T
        return carry

    lax.fori_loop(0, tiles, turn, 0)
    wide = hidden // PARTS

    def add_rows(source, init):
        for o in range(CORES):
            base = ((source * CORES + o) * CODE).astype(F32)
            pick_x[:, o * LANES:(o + 1) * LANES] = onehot(codes[...] == lane + base)
        rows = pl.ds(pl.multiple_of(source * CORES * STRIDE, CORES * STRIDE), CORES * STRIDE)

        def part(k, c):
            cols = pl.ds(pl.multiple_of(k * wide, wide), wide)
            term = jnp.dot(pick_x[...], got[rows, cols], preferred_element_type=F32)
            if init:
                xs[:, cols] = term
            else:
                xs[:, cols] += term
            return c

        lax.fori_loop(0, hidden // wide, part, 0)

    def from_sib(source):
        d = source * CORES + 1 - core
        remote(slot(d), slot(d), fsend.at[3], frecv.at[d], sib).wait_recv()

    shared = []

    def share(k, source):
        d = dev(source)
        copy = remote(slot(d), slot(d), fsend.at[5 + k], frecv.at[d], sib)
        copy.wait_recv()
        copy.start()
        shared.append(copy)

    own.wait()
    from_sib(chip)
    add_rows(chip, True)
    to_far.wait_recv()
    passed = remote(relay, slot(dev(behind)), fsend.at[4], frecv.at[dev(behind)], dev(ahead))
    passed.start()
    share(0, ahead)
    share(1, behind)
    for source in (behind, ahead):
        from_sib(source)
        add_rows(source, False)
    share(2, far)
    from_sib(far)
    add_rows(far, False)
    dy_in.wait()

    gain = gain_ref[...].astype(F32).reshape(1, hidden)
    columns = range(0, hidden, LANES)

    def mine(t):
        return dx.at[pl.ds(pl.multiple_of(core * tokens + t * TILE, TILE), TILE)]

    def swap(t):
        return remote(mine(t), mine(t), tsend.at[t], trecv.at[t], sib)

    def norm_tile(t, carry):
        here = pl.ds(pl.multiple_of(t * TILE, TILE), TILE)
        there = pl.ds(pl.multiple_of(core * tokens + t * TILE, TILE), TILE)
        acc = jnp.zeros((TILE, LANES), F32)
        for c in columns:
            h = xs[here, c:c + LANES]
            acc += h * h
        r = lax.rsqrt(jnp.sum(acc, axis=-1, keepdims=True) / hidden + RMS_EPS)
        r = jnp.broadcast_to(r, (TILE, LANES))
        acc = jnp.zeros((TILE, LANES), F32)
        for c in columns:
            xh = xs[here, c:c + LANES] * r
            gain_c = gain[:, c:c + LANES]
            y[here, c:c + LANES] = (xh.astype(BF16).astype(F32) * gain_c).astype(BF16)
            g = dy[here, c:c + LANES].astype(F32)
            part = g * xh
            acc += g * gain_c * xh
            dgacc[:, c:c + LANES] += jnp.sum(part.reshape(TILE // 8, 8, LANES), axis=0)
        mean = jnp.broadcast_to(jnp.sum(acc, axis=-1, keepdims=True) / hidden, (TILE, LANES))
        for c in columns:
            xh = xs[here, c:c + LANES] * r
            u = dy[here, c:c + LANES].astype(F32) * gain[:, c:c + LANES]
            dx[there, c:c + LANES] = (r * (u - xh * mean)).astype(BF16)
        swap(t).start()
        return carry

    lax.fori_loop(0, tiles, norm_tile, 0)
    y_copy = pltpu.make_async_copy(y, y_hbm, local.at[2])
    y_copy.start()

    dgs[me] = jnp.sum(dgacc[...], axis=0, keepdims=True)
    for k in range(1, n):
        remote(dgs.at[me], dgs.at[me], gsend.at[k], grecv.at[k], lax.rem(me + k, n)).start()

    def swapped(t, carry):
        swap(t).wait()
        return carry

    lax.fori_loop(0, tiles, swapped, 0)

    place = lax.broadcasted_iota(jnp.int32, (LANES, CORES * tokens), 0)

    def picks(dest):
        return onehot((place + dev(dest) * CODE).astype(F32) == code_ref[1:2, :])

    def sums(q, pick, k):
        cols = pl.ds(pl.multiple_of(k * wide, wide), wide)
        total = jnp.dot(pick, dx[:, cols], preferred_element_type=F32)
        psum[q, k] = total[:MULTI]
        pone[q, k] = total[MULTI:].astype(BF16)

    def all_sums(q, dest):
        pick = picks(dest)

        def part(k, c):
            sums(q, pick, k)
            return c

        lax.fori_loop(0, PARTS, part, 0)

    first, relays = [], []
    pick = picks(far)
    for k in range(PARTS):
        sums(0, pick, k)
        for w, (mine_, relay_) in enumerate(((psum, rsum), (pone, rone))):
            first.append(remote(mine_.at[0, k], relay_.at[k], psend.at[w, 0, k], precv.at[w, 0, k], dev(ahead)))
            first[-1].start()

    def back(q, dest, sem):
        out = []
        for w, (mine_, theirs) in enumerate(((psum, gsum), (pone, gone))):
            out.append(remote(mine_.at[q], theirs.at[chip], bsend.at[w, sem], brecv.at[w, chip], dev(dest)))
            out[-1].start()
        return out

    all_sums(1, behind)
    direct = back(1, behind, 0)
    all_sums(2, ahead)
    direct += back(2, ahead, 1)
    all_sums(3, chip)

    def merge(source, multi, single, init):
        index = kmap_ref[pl.ds(source, 1), :]
        pick = onehot(lax.broadcasted_iota(jnp.int32, (UNION, 2 * LANES), 0).astype(F32) == index)
        pad = jnp.zeros((2 * LANES - 3 * MULTI - SINGLE, wide), F32)

        def part(k, c):
            cols = pl.ds(pl.multiple_of(k * wide, wide), wide)
            p = multi[k]
            high = jnp.clip(p, -BF16_MAX, BF16_MAX).astype(BF16).astype(F32)
            rest = p - high
            mid = rest.astype(BF16).astype(F32)
            stack = jnp.concatenate([high, single[k].astype(F32), mid, rest - mid, pad], axis=0).astype(BF16)
            term = jnp.dot(pick, stack, preferred_element_type=F32)
            if init:
                merged[:, cols] = term
            else:
                merged[:, cols] += term
            return c

        lax.fori_loop(0, PARTS, part, 0)

    for k in range(PARTS):
        for w, (relay_, theirs) in enumerate(((rsum, gsum), (rone, gone))):
            first[2 * k + w].wait_recv()
            relays.append(remote(relay_.at[k], theirs.at[behind, k], psend.at[w, 1, k], precv.at[w, 1, k], dev(ahead)))
            relays[-1].start()
    merge(chip, psum.at[3], pone.at[3], True)

    for k in range(1, n):
        remote(dgs.at[me], dgs.at[lax.rem(me - k + n, n)], gsend.at[k], grecv.at[k], sib).wait()
    total = dgs[0]
    for k in range(1, n):
        total = total + dgs[k]
    dg_ref[...] = total

    for source in (ahead, behind):
        for w, (mine_, theirs) in enumerate(((psum, gsum), (pone, gone))):
            remote(mine_.at[0], theirs.at[source], bsend.at[w, 0], brecv.at[w, source], sib).wait_recv()
        merge(source, gsum.at[source], gone.at[source], False)
    for copy in relays:
        copy.wait_recv()
    merge(far, gsum.at[far], gone.at[far], False)
    for copy in (to_far, to_behind, to_ahead, to_sib, passed, *shared, *first, *direct, *relays):
        copy.wait_send()
    y_copy.wait()


def write_kernel(uid_s, merged_ref, y_hbm, dg_ref, out, y_out, dg_out, y, buffers, sem, sem_y):
    slots, tile, _ = buffers.shape
    steps = out.shape[0] // tile
    y_in = pltpu.make_async_copy(y_hbm, y, sem_y.at[0])
    y_back = pltpu.make_async_copy(y, y_out, sem_y.at[1])
    y_in.start()
    dg_out[...] = dg_ref[...]

    def send(i):
        slot = lax.rem(i, slots)
        rows = pl.ds(pl.multiple_of(i * tile, tile), tile)
        return pltpu.make_async_copy(buffers.at[slot], out.at[rows], sem.at[slot])

    def fill(i, p):
        slot = lax.rem(i, slots)

        @pl.when(i >= slots)
        def _():
            send(i - slots).wait()

        buffers[slot] = jnp.zeros(buffers.shape[1:], F32)

        def put(p):
            buffers[slot, pl.ds(uid_s[0, p] - i * tile, 1), :] = merged_ref[pl.ds(p, 1), :]
            return p + 1

        p = lax.while_loop(lambda p: uid_s[0, p] < (i + 1) * tile, put, p)
        send(i).start()
        return p

    p = lax.fori_loop(0, slots, fill, 0)
    y_in.wait()
    y_back.start()
    lax.fori_loop(slots, steps, fill, p)
    for i in range(steps - slots, steps):
        send(i).wait()
    y_back.wait()


def write_out(rows, uid, merged, y, dg):
    tokens, hidden = y.shape
    tile = next(t for t in range(160, 0, -8) if rows % t == 0)
    slots = min(8, rows // tile)
    hbm = pl.BlockSpec(memory_space=pl.ANY)
    vm = pl.BlockSpec(memory_space=pltpu.VMEM)
    return pl.pallas_call(
        write_kernel,
        out_shape=(
            jax.ShapeDtypeStruct((rows, hidden), F32),
            jax.ShapeDtypeStruct((tokens, hidden), BF16),
            jax.ShapeDtypeStruct((1, hidden), F32),
        ),
        in_specs=[pl.BlockSpec(memory_space=pltpu.SMEM), vm, hbm, vm],
        out_specs=(hbm, hbm, vm),
        scratch_shapes=[
            pltpu.VMEM((tokens, hidden), BF16), pltpu.VMEM((slots, tile, hidden), F32),
            pltpu.SemaphoreType.DMA((slots,)), pltpu.SemaphoreType.DMA((2,)),
        ],
        compiler_params=pltpu.CompilerParams(vmem_limit_bytes=60 * 1024 * 1024),
        name='write_out',
    )(uid, merged, y, dg)


def short_path(n, rows, uid, kmap, code, send, gain, grad):
    m = n // CORES
    _, tokens, hidden = grad.shape
    vm = pl.BlockSpec(memory_space=pltpu.VMEM)
    hbm = pl.BlockSpec(memory_space=pl.ANY)
    dma = pltpu.SemaphoreType.DMA
    tiles = tokens // TILE
    y, merged, dg = pl.pallas_call(
        functools.partial(core_kernel, n),
        out_shape=(
            jax.ShapeDtypeStruct((tokens, hidden), BF16),
            jax.ShapeDtypeStruct((UNION, hidden), F32),
            jax.ShapeDtypeStruct((1, hidden), F32),
        ),
        in_specs=[vm, vm, vm, vm, hbm],
        out_specs=(hbm, vm, vm),
        scratch_shapes=[
            pltpu.VMEM((n * STRIDE, hidden), BF16),
            pltpu.VMEM((CAP, hidden), BF16),
            pltpu.VMEM((tokens, hidden), BF16),
            pltpu.VMEM((tokens, hidden), BF16),
            pltpu.VMEM((CORES * tokens, hidden), BF16),
            pltpu.VMEM((tokens, hidden), F32),
            pltpu.VMEM((tokens, LANES), F32),
            pltpu.VMEM((tokens, CORES * LANES), BF16),
            pltpu.VMEM((m, PARTS, MULTI, hidden // PARTS), F32),
            pltpu.VMEM((m, PARTS, SINGLE, hidden // PARTS), BF16),
            pltpu.VMEM((PARTS, MULTI, hidden // PARTS), F32),
            pltpu.VMEM((PARTS, SINGLE, hidden // PARTS), BF16),
            pltpu.VMEM((m, PARTS, MULTI, hidden // PARTS), F32),
            pltpu.VMEM((m, PARTS, SINGLE, hidden // PARTS), BF16),
            pltpu.VMEM((8, hidden), F32),
            pltpu.VMEM((n, 1, hidden), F32),
            dma((8,)), dma((n + 1,)), dma((2, 2)), dma((2, m)), dma((2, 2, PARTS)), dma((2, 2, PARTS)),
            dma((tiles,)), dma((tiles,)), dma((n,)), dma((n,)), dma((3,)),
        ],
        compiler_params=pltpu.CompilerParams(
            collective_id=0, has_side_effects=True, vmem_limit_bytes=52 * 1024 * 1024),
        name='short_path',
    )(send, code, kmap, gain, grad[0])
    table_grad, y, dg = write_out(rows, uid, merged, y, dg)
    return y[None], table_grad, dg[0]


def exchange_kernel(n, per_dest, src, out, send, recv, local):
    me = lax.axis_index('tp')

    def block(d):
        return src.at[d] if per_dest else src

    barrier(n, me)
    own = pltpu.make_async_copy(block(me), out.at[me], local)
    own.start()
    copies = []
    for k in range(1, n):
        peer = lax.rem(me + k, n)
        copies.append(pltpu.make_async_remote_copy(
            src_ref=block(peer), dst_ref=out.at[me], send_sem=send.at[k], recv_sem=recv.at[k],
            device_id={'tp': peer}, device_id_type=MESH))
        copies[-1].start()
    own.wait()
    for copy in copies:
        copy.wait()


def exchange(n, src, collective_id, per_dest):
    shape = src.shape[1:] if per_dest else src.shape
    hbm = pl.BlockSpec(memory_space=pl.ANY)
    dma = pltpu.SemaphoreType.DMA
    return pl.pallas_call(
        functools.partial(exchange_kernel, n, per_dest),
        out_shape=jax.ShapeDtypeStruct((n, *shape), src.dtype),
        in_specs=[hbm],
        out_specs=hbm,
        scratch_shapes=[dma((n,)), dma((n,)), dma(())],
        compiler_params=pltpu.CompilerParams(collective_id=collective_id, has_side_effects=True),
        name=f'exchange{collective_id}',
    )(src)


def norm_pass(embedded, norm_gain, grad_block):
    hidden_f32 = embedded.astype(F32)
    inv_rms = lax.rsqrt(jnp.mean(hidden_f32 * hidden_f32, axis=-1, keepdims=True) + RMS_EPS)
    x_hat = hidden_f32 * inv_rms
    normed = x_hat.astype(BF16) * norm_gain
    grad_f32 = grad_block.astype(F32)
    gain_part = jnp.sum(grad_f32 * x_hat, axis=(0, 1))
    grad_hat = grad_f32 * norm_gain.astype(F32)
    grad_in = (inv_rms * (grad_hat - x_hat * jnp.mean(grad_hat * x_hat, axis=-1, keepdims=True))).astype(BF16)
    return normed, grad_in, gain_part


def dense_path(n, token_ids, table, gain, grad):
    rows, hidden = table.shape
    tokens = grad.shape[1]
    local_ids = token_ids.reshape(-1) - lax.axis_index('tp') * rows
    owned = (local_ids >= 0) & (local_ids < rows)
    looked_up = jnp.take(table, jnp.where(owned, local_ids, 0), axis=0)
    partial = jnp.where(owned[:, None], looked_up, jnp.zeros((), BF16)).reshape(n, tokens, hidden)
    embedded = jnp.sum(exchange(n, partial, 1, True).astype(F32), axis=0).astype(BF16)
    normed, grad_in, gain_part = norm_pass(embedded[None], gain, grad)
    grad_gain = jnp.sum(exchange(n, gain_part.reshape(-1, LANES), 2, False), axis=0).reshape(-1)
    grad_all = exchange(n, grad_in[0], 3, False).reshape(-1, hidden)
    segments = jnp.where(owned, local_ids, rows)
    table_grad = jax.ops.segment_sum(grad_all.astype(F32), segments, num_segments=rows)
    return normed, table_grad, grad_gain


def device_step(n, token_ids, table, gain, grad):
    uid, kmap, code, send, fits = make_lists(token_ids, table, n)
    return lax.cond(
        fits[0, 0] == 1,
        lambda: short_path(n, table.shape[0], uid, kmap, code, send, gain, grad),
        lambda: dense_path(n, token_ids, table, gain, grad),
    )


def solution(mesh):
    n = mesh.shape['tp']
    return jax.shard_map(
        functools.partial(device_step, n), mesh=mesh,
        in_specs=(P('dp', None), P('tp', None), P(None), P('dp', 'tp', None)),
        out_specs=(P('dp', 'tp', None), P(('dp', 'tp'), None), P('dp')), check_vma=False)
```

```python
import functools

import jax
import jax.numpy as jnp
from jax import lax
from jax.experimental import pallas as pl
from jax.experimental.pallas import tpu as pltpu
from jax.sharding import PartitionSpec as P

RMS_EPS = 1e-5
MESH = pl.DeviceIdType.MESH
LANES = 128
CORES = 2
CAP = 112
MULTI = 56
SINGLE = 72
UNION = 240
CODE = 256
STRIDE = 128
PARTS = 4
TILE = 128
BF16_MAX = 3.3895313892515355e38
NT = (((1,), (1,)), ((), ()))
TN = (((0,), (0,)), ((), ()))
F32, BF16 = jnp.float32, jnp.bfloat16


def onehot(mask):
    return jnp.where(mask, 1.0, 0.0).astype(BF16)


def lists_kernel(n, rows, ids_ref, table_hbm, uid_ref, kmap_ref, code_ref, send_ref, fits_ref,
                 table, picked, rank_f, rank_b, rank_u, uid_s, sem):
    m = n // CORES
    width = ids_ref.shape[1] // m
    hb = -(-rows // LANES)
    high = n * hb
    me = lax.axis_index('tp')
    chip = me // CORES
    table_in = pltpu.make_async_copy(table_hbm, table, sem.at[0])
    table_in.start()
    picked[...] = jnp.zeros_like(picked)

    def split(ids):
        owner = jnp.zeros_like(ids)
        for k in range(1, n):
            owner += (ids >= k * rows).astype(jnp.int32)
        local = ids - owner * rows
        return owner, owner * hb + (local >> 7), local & (LANES - 1)

    def hots(hi, lo):
        h = onehot(lax.broadcasted_iota(jnp.int32, (high, width), 0) == hi)
        l = onehot(lax.broadcasted_iota(jnp.int32, (LANES, width), 0) == lo)
        return h, l

    a = lax.broadcasted_iota(jnp.int32, (LANES, LANES), 0)
    b = lax.broadcasted_iota(jnp.int32, (LANES, LANES), 1)
    lower, ones = onehot(a < b), jnp.ones((LANES, LANES), BF16)
    ra = lax.broadcasted_iota(jnp.int32, (high, high), 0)
    rb = lax.broadcasted_iota(jnp.int32, (high, high), 1)
    first = jnp.zeros_like(ra)
    for k in range(1, n):
        first += jnp.where(ra >= k * hb, hb, 0)
    before = onehot((rb < ra) & (rb >= first))

    def ahead_of(mask):
        present = onehot(mask)
        inside = jnp.dot(present, lower, preferred_element_type=F32)
        total = jnp.dot(present, ones, preferred_element_type=F32).astype(BF16)
        return inside + jnp.dot(before, total, preferred_element_type=F32)

    def over(mask, rank, cap):
        return jnp.where(mask & (rank > cap - 0.5), 1.0, 0.0)

    union = jnp.zeros((high, LANES), F32)
    bad = jnp.zeros((high, LANES), F32)
    for j in range(m):
        _, hi, lo = split(ids_ref[:, j * width:(j + 1) * width])
        h, l = hots(hi, lo)
        count = lax.dot_general(h, l, NT, preferred_element_type=F32)
        union += count
        here, many = count > 0.5, count > 1.5
        all_before, many_before = ahead_of(here), ahead_of(many)
        one_before = all_before - many_before
        bad += over(here, all_before, CAP) + over(many, many_before, MULTI) + over(count == 1.0, one_before, SINGLE)
        back = jnp.where(many, many_before, one_before + MULTI)
        rank_f[j] = jnp.where(here, jnp.minimum(all_before, CODE - 1.0), -1.0)
        rank_b[j] = jnp.where(here, jnp.minimum(back, CODE - 1.0), -1.0)
    here = union > 0.5
    all_before = ahead_of(here)
    bad += over(here, all_before, UNION)
    rank_u[...] = jnp.where(here, jnp.minimum(all_before, CODE - 1.0), -1.0)
    fits_ref[0, 0] = (jnp.max(bad) < 0.5).astype(jnp.int32)

    block = pl.ds(pl.multiple_of(me * hb, hb), hb)
    of_union = rank_u[block, :]
    lane = lax.broadcasted_iota(jnp.int32, (1, LANES), 1)
    every = jnp.ones((8, LANES), F32)

    def places(height):
        return lax.broadcasted_iota(jnp.int32, (height, LANES), 0).astype(F32)

    def as_row(found):
        return lax.dot_general(every, found, NT, preferred_element_type=F32, precision=lax.Precision.HIGHEST)[:1, :]

    want = places(CODE)
    found = jnp.zeros((CODE, LANES), F32)
    for k in range(hb):
        found += jnp.where(of_union[k:k + 1, :] == want, (k * LANES + lane).astype(F32), 0.0)
    length = jnp.max(of_union) + 1.0
    place = lax.broadcasted_iota(jnp.int32, (1, CODE), 1).astype(F32)
    uid_ref[...] = jnp.full(uid_ref.shape, rows, jnp.int32)
    uid_ref[:1, :] = jnp.where((place < length) & (place < UNION), as_row(found), float(rows)).astype(jnp.int32)
    uid_in = pltpu.make_async_copy(uid_ref, uid_s, sem.at[1])
    uid_in.start()

    owner, hi, lo = split(ids_ref[:, pl.ds(pl.multiple_of(chip * width, width), width)])
    h, l = hots(hi, lo)
    l = l.astype(F32)
    for k, rank in enumerate((rank_f, rank_b)):
        found = lax.dot_general(rank[chip].astype(BF16), h, TN, preferred_element_type=F32)
        code_ref[k:k + 1, :] = owner.astype(F32) * CODE + jnp.sum(found * l, axis=0, keepdims=True)

    want = places(LANES)
    spread = []
    for j in range(m):
        fwd, back = rank_f[j, block, :], rank_b[j, block, :]
        found_f = jnp.zeros((CAP, LANES), F32)
        found_b = jnp.zeros((LANES, LANES), F32)
        for k in range(hb):
            u = of_union[k:k + 1, :]
            found_f += jnp.where(fwd[k:k + 1, :] == want[:CAP], u, 0.0)
            found_b += jnp.where(back[k:k + 1, :] == want, u + 1.0, 0.0)
        of_slot = jnp.sum(found_f, axis=1, keepdims=True)
        spread.append(onehot(lax.broadcasted_iota(jnp.int32, (CAP, CODE), 1).astype(F32) == of_slot))
        row = as_row(found_b) - 1.0
        again = jnp.where(lane < MULTI, row, jnp.where(lane < 2 * MULTI, pltpu.roll(row, MULTI, 1), -1.0))
        kmap_ref[j:j + 1, :] = jnp.concatenate([row, again], axis=1)

    uid_in.wait()
    table_in.wait()
    pack, eight = 16, 8
    sublane = lax.broadcasted_iota(jnp.int32, (eight, table.shape[2]), 0)
    groups = jnp.minimum((length.astype(jnp.int32) + pack - 1) // pack, UNION // pack)

    def pick(q, carry):
        halves = []
        for half in range(pack // eight):
            acc = jnp.zeros(sublane.shape, F32)
            for k in range(eight):
                v = jnp.minimum(uid_s[0, q * pack + half * eight + k], rows - 1)
                tile = table[v // eight].astype(F32)
                turned = pltpu.roll(tile, lax.rem(k + eight - lax.rem(v, eight), eight), 0)
                acc = jnp.where(sublane == k, turned, acc)
            halves.append(acc)
        picked[pl.ds(pl.multiple_of(q * pack, pack), pack), :] = jnp.concatenate(halves, axis=0).astype(BF16)
        return carry

    lax.fori_loop(0, groups, pick, 0)
    spread = jnp.concatenate(spread, axis=0)
    for c in range(0, table.shape[2], CODE):
        rows_out = jnp.dot(spread, picked[:, c:c + CODE], preferred_element_type=F32).astype(BF16)
        for j in range(m):
            send_ref[j, :, c:c + CODE] = rows_out[j * CAP:(j + 1) * CAP]


def make_lists(token_ids, table, n):
    m = n // CORES
    rows, hidden = table.shape
    hb = -(-rows // LANES)
    vm = pl.BlockSpec(memory_space=pltpu.VMEM)
    return pl.pallas_call(
        functools.partial(lists_kernel, n, rows),
        out_shape=(
            jax.ShapeDtypeStruct((8, CODE), jnp.int32),
            jax.ShapeDtypeStruct((m, 2 * LANES), F32),
            jax.ShapeDtypeStruct((2, token_ids.shape[1] // m), F32),
            jax.ShapeDtypeStruct((m, CAP, hidden), BF16),
            jax.ShapeDtypeStruct((1, 1), jnp.int32),
        ),
        in_specs=[vm, pl.BlockSpec(memory_space=pl.ANY)],
        out_specs=(vm, vm, vm, vm, pl.BlockSpec(memory_space=pltpu.SMEM)),
        scratch_shapes=[
            pltpu.VMEM((rows // 8, 8, hidden), BF16),
            pltpu.VMEM((CODE, hidden), BF16),
            pltpu.VMEM((m, n * hb, LANES), F32),
            pltpu.VMEM((m, n * hb, LANES), F32),
            pltpu.VMEM((n * hb, LANES), F32),
            pltpu.SMEM((8, CODE), jnp.int32),
            pltpu.SemaphoreType.DMA((2,)),
        ],
        compiler_params=pltpu.CompilerParams(vmem_limit_bytes=44 * 1024 * 1024),
        name='lists',
    )(token_ids, table.reshape(rows // 8, 8, hidden))


def barrier(n, me):
    sem = pltpu.get_barrier_semaphore()
    for k in range(1, n):
        pl.semaphore_signal(sem, inc=1, device_id={'tp': lax.rem(me + k, n)}, device_id_type=MESH)
    pl.semaphore_wait(sem, n - 1)


def core_kernel(n, rows_ref, code_ref, kmap_ref, gain_ref, dy_hbm, y, merged, dg_ref,
                got, relay, dy, dx, xs, codes, pick_x, psum, pone, rsum, rone, gsum, gone, dgacc, dgs,
                fsend, frecv, bsend, brecv, psend, precv, tsend, trecv, gsend, grecv, local):
    m = n // CORES
    tokens, hidden = dy_hbm.shape
    tiles = tokens // TILE
    me = lax.axis_index('tp')
    chip, core = me // CORES, lax.rem(me, CORES)
    step = 1 - 2 * core
    ahead, behind, far = (lax.rem(chip + step + m, m), lax.rem(chip - step + m, m), lax.rem(chip + 2, m))
    sib = chip * CORES + 1 - core

    def dev(c):
        return c * CORES + core

    def remote(src, dst, s, r, d):
        return pltpu.make_async_remote_copy(
            src_ref=src, dst_ref=dst, send_sem=s, recv_sem=r, device_id={'tp': d}, device_id_type=MESH)

    def slot(d):
        return got.at[pl.ds(pl.multiple_of(d * STRIDE, STRIDE), CAP)]

    dy_in = pltpu.make_async_copy(dy_hbm, dy, local.at[0])
    dy_in.start()
    own = pltpu.make_async_copy(rows_ref.at[chip], slot(me), local.at[1])
    own.start()
    barrier(n, me)

    to_far = remote(rows_ref.at[far], relay, fsend.at[0], frecv.at[n], dev(ahead))
    to_far.start()
    to_behind = remote(rows_ref.at[behind], slot(me), fsend.at[2], frecv.at[me], dev(behind))
    to_behind.start()
    to_ahead = remote(rows_ref.at[ahead], slot(me), fsend.at[1], frecv.at[me], dev(ahead))
    to_ahead.start()
    to_sib = remote(rows_ref.at[chip], slot(me), fsend.at[3], frecv.at[me], sib)
    to_sib.start()

    lane = lax.broadcasted_iota(jnp.int32, (1, LANES), 1).astype(F32)
    for d in range(n):
        got[d * STRIDE + CAP:(d + 1) * STRIDE, :] = jnp.zeros((STRIDE - CAP, hidden), BF16)
    dgacc[...] = jnp.zeros_like(dgacc)

    def turn(t, carry):
        at = pl.multiple_of(core * tokens + t * TILE, TILE)
        codes[pl.ds(pl.multiple_of(t * TILE, TILE), TILE), :] = jnp.broadcast_to(
            code_ref[:1, pl.ds(at, TILE)], (LANES, TILE)).T
        return carry

    lax.fori_loop(0, tiles, turn, 0)
    wide = hidden // PARTS

    def add_rows(source, init):
        for o in range(CORES):
            base = ((source * CORES + o) * CODE).astype(F32)
            pick_x[:, o * LANES:(o + 1) * LANES] = onehot(codes[...] == lane + base)
        rows = pl.ds(pl.multiple_of(source * CORES * STRIDE, CORES * STRIDE), CORES * STRIDE)

        def part(k, c):
            cols = pl.ds(pl.multiple_of(k * wide, wide), wide)
            term = jnp.dot(pick_x[...], got[rows, cols], preferred_element_type=F32)
            if init:
                xs[:, cols] = term
            else:
                xs[:, cols] += term
            return c

        lax.fori_loop(0, hidden // wide, part, 0)

    def from_sib(source):
        d = source * CORES + 1 - core
        remote(slot(d), slot(d), fsend.at[3], frecv.at[d], sib).wait_recv()

    shared = []

    def share(k, source):
        d = dev(source)
        copy = remote(slot(d), slot(d), fsend.at[5 + k], frecv.at[d], sib)
        copy.wait_recv()
        copy.start()
        shared.append(copy)

    own.wait()
    from_sib(chip)
    add_rows(chip, True)
    to_far.wait_recv()
    passed = remote(relay, slot(dev(behind)), fsend.at[4], frecv.at[dev(behind)], dev(ahead))
    passed.start()
    share(0, ahead)
    share(1, behind)
    for source in (behind, ahead):
        from_sib(source)
        add_rows(source, False)
    share(2, far)
    from_sib(far)
    add_rows(far, False)
    dy_in.wait()

    gain = gain_ref[...].astype(F32).reshape(1, hidden)
    columns = range(0, hidden, LANES)

    def mine(t):
        return dx.at[pl.ds(pl.multiple_of(core * tokens + t * TILE, TILE), TILE)]

    def swap(t):
        return remote(mine(t), mine(t), tsend.at[t], trecv.at[t], sib)

    def norm_tile(t, carry):
        here = pl.ds(pl.multiple_of(t * TILE, TILE), TILE)
        there = pl.ds(pl.multiple_of(core * tokens + t * TILE, TILE), TILE)
        acc = jnp.zeros((TILE, LANES), F32)
        for c in columns:
            h = xs[here, c:c + LANES]
            acc += h * h
        r = lax.rsqrt(jnp.sum(acc, axis=-1, keepdims=True) / hidden + RMS_EPS)
        r = jnp.broadcast_to(r, (TILE, LANES))
        acc = jnp.zeros((TILE, LANES), F32)
        for c in columns:
            xh = xs[here, c:c + LANES] * r
            gain_c = gain[:, c:c + LANES]
            y[here, c:c + LANES] = (xh.astype(BF16).astype(F32) * gain_c).astype(BF16)
            g = dy[here, c:c + LANES].astype(F32)
            part = g * xh
            acc += g * gain_c * xh
            dgacc[:, c:c + LANES] += jnp.sum(part.reshape(TILE // 8, 8, LANES), axis=0)
        mean = jnp.broadcast_to(jnp.sum(acc, axis=-1, keepdims=True) / hidden, (TILE, LANES))
        for c in columns:
            xh = xs[here, c:c + LANES] * r
            u = dy[here, c:c + LANES].astype(F32) * gain[:, c:c + LANES]
            dx[there, c:c + LANES] = (r * (u - xh * mean)).astype(BF16)
        swap(t).start()
        return carry

    lax.fori_loop(0, tiles, norm_tile, 0)

    dgs[me] = jnp.sum(dgacc[...], axis=0, keepdims=True)
    for k in range(1, n):
        remote(dgs.at[me], dgs.at[me], gsend.at[k], grecv.at[k], lax.rem(me + k, n)).start()

    def swapped(t, carry):
        swap(t).wait()
        return carry

    lax.fori_loop(0, tiles, swapped, 0)

    place = lax.broadcasted_iota(jnp.int32, (LANES, CORES * tokens), 0)

    def picks(dest):
        return onehot((place + dev(dest) * CODE).astype(F32) == code_ref[1:2, :])

    def sums(q, pick, k):
        cols = pl.ds(pl.multiple_of(k * wide, wide), wide)
        total = jnp.dot(pick, dx[:, cols], preferred_element_type=F32)
        psum[q, k] = total[:MULTI]
        pone[q, k] = total[MULTI:].astype(BF16)

    def all_sums(q, dest):
        pick = picks(dest)

        def part(k, c):
            sums(q, pick, k)
            return c

        lax.fori_loop(0, PARTS, part, 0)

    first, relays = [], []
    pick = picks(far)
    for k in range(PARTS):
        sums(0, pick, k)
        for w, (mine_, relay_) in enumerate(((psum, rsum), (pone, rone))):
            first.append(remote(mine_.at[0, k], relay_.at[k], psend.at[w, 0, k], precv.at[w, 0, k], dev(ahead)))
            first[-1].start()

    def back(q, dest, sem):
        out = []
        for w, (mine_, theirs) in enumerate(((psum, gsum), (pone, gone))):
            out.append(remote(mine_.at[q], theirs.at[chip], bsend.at[w, sem], brecv.at[w, chip], dev(dest)))
            out[-1].start()
        return out

    all_sums(1, behind)
    direct = back(1, behind, 0)
    all_sums(2, ahead)
    direct += back(2, ahead, 1)
    all_sums(3, chip)

    def merge(source, multi, single, init):
        index = kmap_ref[pl.ds(source, 1), :]
        pick = onehot(lax.broadcasted_iota(jnp.int32, (UNION, 2 * LANES), 0).astype(F32) == index)
        pad = jnp.zeros((2 * LANES - 3 * MULTI - SINGLE, wide), F32)

        def part(k, c):
            cols = pl.ds(pl.multiple_of(k * wide, wide), wide)
            p = multi[k]
            high = jnp.clip(p, -BF16_MAX, BF16_MAX).astype(BF16).astype(F32)
            rest = p - high
            mid = rest.astype(BF16).astype(F32)
            stack = jnp.concatenate([high, single[k].astype(F32), mid, rest - mid, pad], axis=0).astype(BF16)
            term = jnp.dot(pick, stack, preferred_element_type=F32)
            if init:
                merged[:, cols] = term
            else:
                merged[:, cols] += term
            return c

        lax.fori_loop(0, PARTS, part, 0)

    for k in range(PARTS):
        for w, (relay_, theirs) in enumerate(((rsum, gsum), (rone, gone))):
            first[2 * k + w].wait_recv()
            relays.append(remote(relay_.at[k], theirs.at[behind, k], psend.at[w, 1, k], precv.at[w, 1, k], dev(ahead)))
            relays[-1].start()
    merge(chip, psum.at[3], pone.at[3], True)

    for k in range(1, n):
        remote(dgs.at[me], dgs.at[lax.rem(me - k + n, n)], gsend.at[k], grecv.at[k], sib).wait()
    total = dgs[0]
    for k in range(1, n):
        total = total + dgs[k]
    dg_ref[...] = total

    for source in (ahead, behind):
        for w, (mine_, theirs) in enumerate(((psum, gsum), (pone, gone))):
            remote(mine_.at[0], theirs.at[source], bsend.at[w, 0], brecv.at[w, source], sib).wait_recv()
        merge(source, gsum.at[source], gone.at[source], False)
    for copy in relays:
        copy.wait_recv()
    merge(far, gsum.at[far], gone.at[far], False)
    for copy in (to_far, to_behind, to_ahead, to_sib, passed, *shared, *first, *direct, *relays):
        copy.wait_send()


def write_kernel(uid_s, merged_ref, y, dg_ref, out, y_out, dg_out, buffers, sem, sem_y):
    slots, tile, _ = buffers.shape
    steps = out.shape[0] // tile
    y_back = pltpu.make_async_copy(y, y_out, sem_y)
    y_back.start()
    dg_out[...] = dg_ref[...]

    def send(i):
        slot = lax.rem(i, slots)
        rows = pl.ds(pl.multiple_of(i * tile, tile), tile)
        return pltpu.make_async_copy(buffers.at[slot], out.at[rows], sem.at[slot])

    def fill(i, p):
        slot = lax.rem(i, slots)

        @pl.when(i >= slots)
        def _():
            send(i - slots).wait()

        buffers[slot] = jnp.zeros(buffers.shape[1:], F32)

        def put(p):
            buffers[slot, pl.ds(uid_s[0, p] - i * tile, 1), :] = merged_ref[pl.ds(p, 1), :]
            return p + 1

        p = lax.while_loop(lambda p: uid_s[0, p] < (i + 1) * tile, put, p)
        send(i).start()
        return p

    lax.fori_loop(0, steps, fill, 0)
    for i in range(steps - slots, steps):
        send(i).wait()
    y_back.wait()


def write_out(rows, uid, merged, y, dg):
    tokens, hidden = y.shape
    tile = next(t for t in range(160, 0, -8) if rows % t == 0)
    slots = min(8, rows // tile)
    hbm = pl.BlockSpec(memory_space=pl.ANY)
    vm = pl.BlockSpec(memory_space=pltpu.VMEM)
    return pl.pallas_call(
        write_kernel,
        out_shape=(
            jax.ShapeDtypeStruct((rows, hidden), F32),
            jax.ShapeDtypeStruct((tokens, hidden), BF16),
            jax.ShapeDtypeStruct((1, hidden), F32),
        ),
        in_specs=[pl.BlockSpec(memory_space=pltpu.SMEM), vm, vm, vm],
        out_specs=(hbm, hbm, vm),
        scratch_shapes=[
            pltpu.VMEM((slots, tile, hidden), F32), pltpu.SemaphoreType.DMA((slots,)), pltpu.SemaphoreType.DMA(()),
        ],
        compiler_params=pltpu.CompilerParams(vmem_limit_bytes=24 * 1024 * 1024),
        name='write_out',
    )(uid, merged, y, dg)


def short_path(n, rows, uid, kmap, code, send, gain, grad):
    m = n // CORES
    _, tokens, hidden = grad.shape
    vm = pl.BlockSpec(memory_space=pltpu.VMEM)
    hbm = pl.BlockSpec(memory_space=pl.ANY)
    dma = pltpu.SemaphoreType.DMA
    tiles = tokens // TILE
    y, merged, dg = pl.pallas_call(
        functools.partial(core_kernel, n),
        out_shape=(
            jax.ShapeDtypeStruct((tokens, hidden), BF16),
            jax.ShapeDtypeStruct((UNION, hidden), F32),
            jax.ShapeDtypeStruct((1, hidden), F32),
        ),
        in_specs=[vm, vm, vm, vm, hbm],
        out_specs=(vm, vm, vm),
        scratch_shapes=[
            pltpu.VMEM((n * STRIDE, hidden), BF16),
            pltpu.VMEM((CAP, hidden), BF16),
            pltpu.VMEM((tokens, hidden), BF16),
            pltpu.VMEM((CORES * tokens, hidden), BF16),
            pltpu.VMEM((tokens, hidden), F32),
            pltpu.VMEM((tokens, LANES), F32),
            pltpu.VMEM((tokens, CORES * LANES), BF16),
            pltpu.VMEM((m, PARTS, MULTI, hidden // PARTS), F32),
            pltpu.VMEM((m, PARTS, SINGLE, hidden // PARTS), BF16),
            pltpu.VMEM((PARTS, MULTI, hidden // PARTS), F32),
            pltpu.VMEM((PARTS, SINGLE, hidden // PARTS), BF16),
            pltpu.VMEM((m, PARTS, MULTI, hidden // PARTS), F32),
            pltpu.VMEM((m, PARTS, SINGLE, hidden // PARTS), BF16),
            pltpu.VMEM((8, hidden), F32),
            pltpu.VMEM((n, 1, hidden), F32),
            dma((8,)), dma((n + 1,)), dma((2, 2)), dma((2, m)), dma((2, 2, PARTS)), dma((2, 2, PARTS)),
            dma((tiles,)), dma((tiles,)), dma((n,)), dma((n,)), dma((2,)),
        ],
        compiler_params=pltpu.CompilerParams(
            collective_id=0, has_side_effects=True, vmem_limit_bytes=44 * 1024 * 1024),
        name='short_path',
    )(send, code, kmap, gain, grad[0])
    table_grad, y, dg = write_out(rows, uid, merged, y, dg)
    return y[None], table_grad, dg[0]


def exchange_kernel(n, per_dest, src, out, send, recv, local):
    me = lax.axis_index('tp')

    def block(d):
        return src.at[d] if per_dest else src

    barrier(n, me)
    own = pltpu.make_async_copy(block(me), out.at[me], local)
    own.start()
    copies = []
    for k in range(1, n):
        peer = lax.rem(me + k, n)
        copies.append(pltpu.make_async_remote_copy(
            src_ref=block(peer), dst_ref=out.at[me], send_sem=send.at[k], recv_sem=recv.at[k],
            device_id={'tp': peer}, device_id_type=MESH))
        copies[-1].start()
    own.wait()
    for copy in copies:
        copy.wait()


def exchange(n, src, collective_id, per_dest):
    shape = src.shape[1:] if per_dest else src.shape
    hbm = pl.BlockSpec(memory_space=pl.ANY)
    dma = pltpu.SemaphoreType.DMA
    return pl.pallas_call(
        functools.partial(exchange_kernel, n, per_dest),
        out_shape=jax.ShapeDtypeStruct((n, *shape), src.dtype),
        in_specs=[hbm],
        out_specs=hbm,
        scratch_shapes=[dma((n,)), dma((n,)), dma(())],
        compiler_params=pltpu.CompilerParams(collective_id=collective_id, has_side_effects=True),
        name=f'exchange{collective_id}',
    )(src)


def norm_pass(embedded, norm_gain, grad_block):
    hidden_f32 = embedded.astype(F32)
    inv_rms = lax.rsqrt(jnp.mean(hidden_f32 * hidden_f32, axis=-1, keepdims=True) + RMS_EPS)
    x_hat = hidden_f32 * inv_rms
    normed = x_hat.astype(BF16) * norm_gain
    grad_f32 = grad_block.astype(F32)
    gain_part = jnp.sum(grad_f32 * x_hat, axis=(0, 1))
    grad_hat = grad_f32 * norm_gain.astype(F32)
    grad_in = (inv_rms * (grad_hat - x_hat * jnp.mean(grad_hat * x_hat, axis=-1, keepdims=True))).astype(BF16)
    return normed, grad_in, gain_part


def dense_path(n, token_ids, table, gain, grad):
    rows, hidden = table.shape
    tokens = grad.shape[1]
    local_ids = token_ids.reshape(-1) - lax.axis_index('tp') * rows
    owned = (local_ids >= 0) & (local_ids < rows)
    looked_up = jnp.take(table, jnp.where(owned, local_ids, 0), axis=0)
    partial = jnp.where(owned[:, None], looked_up, jnp.zeros((), BF16)).reshape(n, tokens, hidden)
    embedded = jnp.sum(exchange(n, partial, 1, True).astype(F32), axis=0).astype(BF16)
    normed, grad_in, gain_part = norm_pass(embedded[None], gain, grad)
    grad_gain = jnp.sum(exchange(n, gain_part.reshape(-1, LANES), 2, False), axis=0).reshape(-1)
    grad_all = exchange(n, grad_in[0], 3, False).reshape(-1, hidden)
    segments = jnp.where(owned, local_ids, rows)
    table_grad = jax.ops.segment_sum(grad_all.astype(F32), segments, num_segments=rows)
    return normed, table_grad, grad_gain


def device_step(n, token_ids, table, gain, grad):
    uid, kmap, code, send, fits = make_lists(token_ids, table, n)
    return lax.cond(
        fits[0, 0] == 1,
        lambda: short_path(n, table.shape[0], uid, kmap, code, send, gain, grad),
        lambda: dense_path(n, token_ids, table, gain, grad),
    )


def solution(mesh):
    n = mesh.shape['tp']
    return jax.shard_map(
        functools.partial(device_step, n), mesh=mesh,
        in_specs=(P('dp', None), P('tp', None), P(None), P('dp', 'tp', None)),
        out_specs=(P('dp', 'tp', None), P(('dp', 'tp'), None), P('dp')), check_vma=False)
```
